32 devices in a mesh: group: 2 (over y), seq: 8 (over z, x), head: 2 (over core).
Axes of the slice: x: 2, y: 2, z: 4, core: 2. Of those that a mesh axis runs over, the one named last changes fastest.
Arguments:
- response_query: bfloat16 [16, 128, 4096], P('group', 'seq', 'head'), parts along dimension 0, may hold values from -6 to 6, as said below
- response_key: bfloat16 [16, 128, 512], P('group', 'seq', 'head'), parts along dimension 0, may hold values from -8 to 8, as said below
- response_value: bfloat16 [16, 128, 512], P('group', 'seq', 'head'), parts along dimension 0, may hold values from -6 to 6
- response_grad: bfloat16 [16, 128, 4096], P('group', 'seq', 'head'), parts along dimension 0, may hold values from -6 to 6
- prompt_key: bfloat16 [192, 512], P(('group', 'seq'), 'head'), parts along dimension 0, may hold values from -8 to 8, as said below
- prompt_value: bfloat16 [192, 512], P(('group', 'seq'), 'head'), parts along dimension 0, may hold values from -6 to 6
- lengths: int32 [16], P('group'), parts along dimension 0, may hold values from 1 to 128, 512 in all
- home_rank: int32 [16], P('group'), parts along dimension 0, may hold values from 0 to 7, each once
- prompt_seen: int32 [16], P('group'), parts along dimension 0, may hold values from 24 to 96
Outputs:
- response_output: bfloat16 [16, 128, 4096], P(('group', 'seq'), None, 'head'), parts along dimension 0
- response_query_grad: bfloat16 [16, 128, 4096], P('group', 'seq', 'head'), parts along dimension 0
- response_key_grad: bfloat16 [16, 128, 512], P('group', 'seq', 'head'), parts along dimension 0
- response_value_grad: bfloat16 [16, 128, 512], P('group', 'seq', 'head'), parts along dimension 0
- prompt_key_grad: bfloat16 [192, 512], P(('group', 'seq'), 'head'), parts along dimension 0
- prompt_value_grad: bfloat16 [192, 512], P(('group', 'seq'), 'head'), parts along dimension 0
The draws below stay inside these ranges and needn't reach their ends.
There are 2 independent parts, one for each index of `group`. The reference program is written for one: setup_inputs(seed, part) draws one part's arguments, and reference() takes and returns one part's arrays. A program takes and returns all parts, laid end to end along the dimension named above; each array names one. Nothing has to cross between parts.
Inputs may be any that keep to these rules, and one draw needn't show every extreme that they name: `response_query`: queries are finite. `response_key`: keys are finite. `prompt_key`: keys are finite. `lengths`: some response has exactly 128 tokens. `home_rank`: every index of seq is the home of exactly one response.
All inputs are finite; a program needn't handle non-finite values.
Results may differ from the reference program's by a relative error of at most 0.017.
The reference program's roundings to bfloat16 on the way (of `weights` and `dlogit`) count: a program that leaves them out, or rounds other values in their place, can miss the bound.
Values may be sent and summed in bfloat16 or wider, within the bound.
No kernel may reach another device: no remote copies, remote signals or barrier semaphores. Data moves between devices by JAX's collectives and lax.ppermute only.
A program may use at most 128 MiB of HBM per device.

```python
import math
import jax
import jax.numpy as jnp
import numpy as np
from jax import lax

QHEADS = 32
KVHEADS = 4
HEAD_DIM = 128
MAX_LEN = 128
RESPONSES = 8
PROMPT = 96


def query_rows(key, salt, shape):
    own_key = jax.random.fold_in(key, salt)
    base = jnp.clip(jax.random.normal(jax.random.fold_in(own_key, 1), shape, jnp.float32), -6.0, 6.0)
    return base


def key_rows(key, salt, shape):
    own_key = jax.random.fold_in(key, salt)
    base = jnp.clip(jax.random.normal(jax.random.fold_in(own_key, 1), shape, jnp.float32), -6.0, 6.0)
    return base


def draw_response_query(key, part):
    return query_rows(key, 11, (RESPONSES, MAX_LEN, QHEADS * HEAD_DIM)).astype(jnp.bfloat16)


def draw_response_key(key, part):
    return key_rows(key, 13, (RESPONSES, MAX_LEN, KVHEADS * HEAD_DIM)).astype(jnp.bfloat16)


def draw_prompt_key(key, part):
    return key_rows(key, 14, (PROMPT, KVHEADS * HEAD_DIM)).astype(jnp.bfloat16)


def touch_ends(drawn, key, low, top_value):
    extent = drawn.shape
    spot = [jax.random.randint(jax.random.fold_in(key, axis), (), 0, extent[axis]) for axis in range(len(extent))]
    drawn = drawn.at[tuple(spot)].set(low)
    longest = extent.index(max(extent))
    spot[longest] = (spot[longest] + 1) % extent[longest]
    return drawn.at[tuple(spot)].set(top_value)


def block_levels(key, dims, pieces, smallest, largest):
    level = 1.0
    for dim, blocks in pieces:
        steps = jax.random.uniform(jax.random.fold_in(jax.random.fold_in(key, 6), dim), (blocks,), jnp.float32, smallest / len(pieces), largest / len(pieces))
        level = level * jnp.repeat(jnp.exp(steps), dims[dim] // blocks).reshape((-1,) + (1,) * (len(dims) - 1 - dim))
    return level


def split_up(number_of, total, limit, slope):
    loads = [(1 << 20) // math.isqrt(grade ** slope) + 1 for grade in range(2, number_of + 1)]
    spare, holding = total - limit - (number_of - 1), [1] * (number_of - 1)
    while spare > 0:
        free = [i for i in range(number_of - 1) if holding[i] < limit]
        pool, remaining = sum([loads[i] for i in free]), spare
        for i in free:
            addition = min(limit - holding[i], max(1, remaining * loads[i] // pool), spare)
            holding[i] = holding[i] + addition
            spare = spare - addition
    return np.array([limit] + holding)


def ragged(rng, amount, total, most, slope):
    if amount == 2:
        one = jax.random.randint(rng, (), max(1, total - most), min(most, total - 1) + 1)
        return jnp.stack([one, total - one])
    tallies = jnp.asarray(split_up(amount, total, most, slope), jnp.int32)
    couples = (amount - 1) // 2
    source_of, taker = tallies[1:1 + 2 * couples:2], tallies[2:2 + 2 * couples:2]
    slack = jnp.minimum(source_of - 1, most - taker)
    passed = jax.random.randint(jax.random.fold_in(rng, 1), (couples,), 0, 1 << 20) % (slack + 1)
    tallies = tallies.at[1:1 + 2 * couples:2].set(source_of - passed).at[2:2 + 2 * couples:2].set(taker + passed)
    return tallies[jax.random.permutation(jax.random.fold_in(rng, 2), amount)]


def scatter_about(key, extent, scale, reach, shards=(), held_as=jnp.bfloat16):
    factor_of = block_levels(key, extent, shards, -0.22, 0.18) if shards else 1.0
    values = jax.random.normal(key, extent, jnp.float32) * scale * factor_of
    return jnp.minimum(jnp.maximum(values, -reach), reach).astype(held_as)


def setup_inputs(seed: int = 0, part: int = 0) -> dict:
    keys = jax.random.split(jax.random.key(seed), 10)
    part_splits = jax.random.split(jax.random.fold_in(keys[9], part), 10)
    return {
        "response_query": draw_response_query(jax.random.fold_in(jax.random.fold_in(keys[9], part), 71), part),
        "response_key": draw_response_key(jax.random.fold_in(jax.random.fold_in(keys[9], part), 71), part),
        "response_value": scatter_about(part_splits[2], (RESPONSES, MAX_LEN, KVHEADS * HEAD_DIM), 1.0, 6.0, ((1, 8), (2, 2))),
        "response_grad": scatter_about(part_splits[3], (RESPONSES, MAX_LEN, QHEADS * HEAD_DIM), 1.0, 6.0, ((1, 8), (2, 2))),
        "prompt_key": draw_prompt_key(jax.random.fold_in(jax.random.fold_in(keys[9], part), 71), part),
        "prompt_value": scatter_about(part_splits[5], (PROMPT, KVHEADS * HEAD_DIM), 1.0, 6.0, ((0, 8), (1, 2))),
        "lengths": ragged(part_splits[6], RESPONSES, RESPONSES * MAX_LEN // 2, MAX_LEN, 2).astype(jnp.int32),
        "home_rank": jax.random.permutation(part_splits[7], RESPONSES).astype(jnp.int32),
        "prompt_seen": touch_ends(jax.random.randint(part_splits[8], (RESPONSES,), PROMPT // 4, PROMPT + 1), jax.random.fold_in(part_splits[8], 1), PROMPT // 4, PROMPT).astype(jnp.int32),
    }


NEG_FILL = -1.0e30


def attend(queries, all_keys, all_values, grad_rows, allowed, live_rows, scale_factor):
    row_count = queries.shape[0]
    kv_count = all_keys.shape[1] // HEAD_DIM
    group_size = queries.shape[1] // all_keys.shape[1]
    outputs = []
    query_grads = []
    key_grads = []
    value_grads = []
    for head_index in range(kv_count):
        low = head_index * group_size * HEAD_DIM
        high = (head_index + 1) * group_size * HEAD_DIM
        query_head = queries[:, low:high].reshape(row_count, group_size, HEAD_DIM).astype(jnp.float32)
        key_head = all_keys[:, head_index * HEAD_DIM:(head_index + 1) * HEAD_DIM].astype(jnp.float32)
        value_head = all_values[:, head_index * HEAD_DIM:(head_index + 1) * HEAD_DIM].astype(jnp.float32)
        grad_head = jnp.where(live_rows[:, None], grad_rows[:, low:high], jnp.zeros((), jnp.bfloat16))
        grad_head = grad_head.reshape(row_count, group_size, HEAD_DIM).astype(jnp.float32)
        logits = jnp.einsum("rhd,kd->rhk", query_head, key_head) * scale_factor
        logits = jnp.where(allowed[:, None, :], logits, NEG_FILL)
        row_max = jnp.max(logits, axis=2, keepdims=True)
        log_total = row_max + jnp.log(jnp.sum(jnp.exp(logits - row_max), axis=2, keepdims=True))
        prob = jnp.exp(logits - log_total)
        weights = lax.optimization_barrier(prob.astype(jnp.bfloat16)).astype(jnp.float32)
        mixed = jnp.einsum("rhk,kd->rhd", weights, value_head)
        output_head = jnp.where(live_rows[:, None, None], mixed, 0.0).astype(jnp.bfloat16)
        output_wide = lax.optimization_barrier(output_head).astype(jnp.float32)
        row_dot = jnp.sum(grad_head * output_wide, axis=2, keepdims=True)
        spread = jnp.einsum("rhd,kd->rhk", grad_head, value_head)
        dlogit = lax.optimization_barrier((prob * (spread - row_dot)).astype(jnp.bfloat16)).astype(jnp.float32)
        query_grads.append((jnp.einsum("rhk,kd->rhd", dlogit, key_head) * scale_factor).reshape(row_count, group_size * HEAD_DIM))
        key_grads.append(jnp.einsum("rhk,rhd->kd", dlogit, query_head) * scale_factor)
        value_grads.append(jnp.einsum("rhk,rhd->kd", weights, grad_head))
        outputs.append(output_head.reshape(row_count, group_size * HEAD_DIM))
    return (jnp.concatenate(outputs, axis=1), jnp.concatenate(query_grads, axis=1),
            jnp.concatenate(key_grads, axis=1), jnp.concatenate(value_grads, axis=1))


def reference(response_query, response_key, response_value, response_grad, prompt_key,
              prompt_value, lengths, home_rank, prompt_seen):
    rank_count = home_rank.shape[0]
    rank_ids = jnp.arange(rank_count, dtype=jnp.int32)
    resident = jnp.sum(jnp.where(home_rank[None, :] == rank_ids[:, None], rank_ids[None, :], 0), axis=1).astype(jnp.int32)
    prompt_total = prompt_key.shape[0]
    max_length = response_query.shape[1]
    scale_factor = 1.0 / (HEAD_DIM ** 0.5)
    positions = jnp.arange(max_length, dtype=jnp.int32)
    prompt_cols = jnp.arange(prompt_total, dtype=jnp.int32)

    def one_response(carry, index):
        key_total, value_total = carry
        all_keys = jnp.concatenate([prompt_key, response_key[index]], axis=0)
        all_values = jnp.concatenate([prompt_value, response_value[index]], axis=0)
        seen_part = jnp.broadcast_to(prompt_cols[None, :] < prompt_seen[index], (max_length, prompt_total))
        causal_part = positions[None, :] <= positions[:, None]
        allowed = jnp.concatenate([seen_part, causal_part], axis=1)
        live_rows = positions < lengths[index]
        output, query_grad, key_grad, value_grad = attend(response_query[index], all_keys, all_values,
                                                          response_grad[index], allowed, live_rows, scale_factor)
        carry = (key_total + key_grad[:prompt_total], value_total + value_grad[:prompt_total])
        return carry, (output, query_grad.astype(jnp.bfloat16), key_grad[prompt_total:].astype(jnp.bfloat16),
                       value_grad[prompt_total:].astype(jnp.bfloat16))

    start = (jnp.zeros(prompt_key.shape, jnp.float32), jnp.zeros(prompt_value.shape, jnp.float32))
    (key_total, value_total), stacked = lax.scan(one_response, start, rank_ids)
    outputs, query_grads, key_grads, value_grads = stacked
    return (outputs[resident], query_grads, key_grads, value_grads,
            key_total.astype(jnp.bfloat16), value_total.astype(jnp.bfloat16))
```

```python
import functools

import jax
import jax.numpy as jnp
from jax import lax
from jax.experimental import pallas as pl
from jax.experimental.pallas import tpu as pltpu
from jax.sharding import PartitionSpec as P

HEAD_DIM = 128


NEG_FILL = -1e30
BF16 = jnp.bfloat16
F32 = jnp.float32


def resident_of(home_ref, rank, count):
    found = jnp.int32(0)
    for index in range(count):
        found = jnp.where(home_ref[index] == rank, jnp.int32(index), found)
    return found


def dot(left, right, contract):
    return lax.dot_general(left, right, ((contract[0], contract[1]), ((), ())), preferred_element_type=F32)


def pack_kernel(home_ref, q_ref, k_ref, v_ref, g_ref, pk_ref, pv_ref, *rest, count):
    blocks, prompt, sems = rest[:count], rest[count], rest[count + 1]
    rank = lax.axis_index("seq")
    prompt_rows, kv_width = pk_ref.shape
    q_width = q_ref.shape[2]
    starts = []
    for distance in range(count):
        index = resident_of(home_ref, rank ^ distance, count)
        block = blocks[distance]
        low = 0
        for part, ref in enumerate((q_ref, g_ref, k_ref, v_ref)):
            width = ref.shape[2]
            starts.append(
                pltpu.make_async_copy(
                    ref.at[index], block.at[:, pl.ds(low, width)], sems.at[distance, part]
                )
            )
            starts[-1].start()
            low += width
    prompt[...] = jnp.zeros(prompt.shape, BF16)
    prompt[:prompt_rows, :kv_width] = pk_ref[...]
    prompt[:prompt_rows, kv_width:] = pv_ref[...]
    low = 2 * q_width + 2 * kv_width
    for distance in range(count):
        starts.append(
            pltpu.make_async_copy(
                prompt, blocks[distance].at[:, pl.ds(low, 2 * kv_width)], sems.at[distance, 4]
            )
        )
        starts[-1].start()
    for copy in starts:
        copy.wait()


def attend_kernel(lengths_ref, home_ref, seen_ref, *rest, count, prompt_rows, q_width, kv_width):
    blocks = rest[:count]
    out_ref = rest[count]
    returns = rest[count + 1 : 2 * count + 1]
    x, y, o, in_sems, out_sems = rest[2 * count + 1 :]
    rank = lax.axis_index("seq")
    rows = blocks[0].shape[0]
    total = rows * count
    kv_count = kv_width // HEAD_DIM
    group_size = q_width // kv_width
    scale = 1.0 / HEAD_DIM**0.5
    arrivals = []
    for distance in range(count):
        arrivals.append(
            pltpu.make_async_copy(
                blocks[distance], x.at[pl.ds((rank ^ distance) * rows, rows), :], in_sems.at[distance]
            )
        )
        arrivals[-1].start()
    own = resident_of(home_ref, rank, count)
    length = lengths_ref[own]
    visible = seen_ref[own]
    column = lax.broadcasted_iota(jnp.int32, (total, total), 1)
    position = lax.broadcasted_iota(jnp.int32, (total, total), 0)
    shard_row = column % rows
    prompt_index = column // rows * prompt_rows + shard_row
    allowed = jnp.concatenate(
        [(shard_row < prompt_rows) & (prompt_index < visible), column <= position], axis=1
    )
    live = lax.broadcasted_iota(jnp.int32, (total, HEAD_DIM), 0) < length
    for copy in arrivals:
        copy.wait()
    leaving = []
    for kv in range(kv_count):
        low = 2 * q_width + kv * HEAD_DIM
        keys = jnp.concatenate(
            [x[:, low + 2 * kv_width : low + 2 * kv_width + HEAD_DIM], x[:, low : low + HEAD_DIM]], axis=0
        )
        low += kv_width
        values = jnp.concatenate(
            [x[:, low + 2 * kv_width : low + 2 * kv_width + HEAD_DIM], x[:, low : low + HEAD_DIM]], axis=0
        )
        key_grad = jnp.zeros((2 * total, HEAD_DIM), F32)
        value_grad = jnp.zeros((2 * total, HEAD_DIM), F32)
        for member in range(group_size):
            head = (kv * group_size + member) * HEAD_DIM
            query = x[:, head : head + HEAD_DIM]
            grad = jnp.where(live, x[:, q_width + head : q_width + head + HEAD_DIM], jnp.zeros((), BF16))
            logits = jnp.where(allowed, dot(query, keys, ((1,), (1,))) * scale, NEG_FILL)
            spread = dot(grad, values, ((1,), (1,)))
            raised = jnp.exp(logits - jnp.max(logits, axis=1, keepdims=True))
            prob = raised * (1.0 / jnp.sum(raised, axis=1, keepdims=True))
            weights = prob.astype(BF16)
            output = jnp.where(live, dot(weights, values, ((1,), (0,))), 0.0).astype(BF16)
            o[:, head : head + HEAD_DIM] = output
            row_dot = jnp.sum(grad.astype(F32) * output.astype(F32), axis=1, keepdims=True)
            dlogit = (prob * (spread - row_dot)).astype(BF16)
            y[:, head : head + HEAD_DIM] = (dot(dlogit, keys, ((1,), (0,))) * scale).astype(BF16)
            key_grad += dot(dlogit, query, ((0,), (0,)))
            value_grad += dot(weights, grad, ((0,), (0,)))
        low = q_width + kv * HEAD_DIM
        for part, summed in enumerate((key_grad * scale, value_grad)):
            at = low + part * kv_width
            y[:, at : at + HEAD_DIM] = summed[total:].astype(BF16)
            at += 2 * kv_width
            y[:, at : at + HEAD_DIM] = summed[:total].astype(BF16)
    for distance in range(count):
        leaving.append(
            pltpu.make_async_copy(
                y.at[pl.ds((rank ^ distance) * rows, rows), :], returns[distance], out_sems.at[distance]
            )
        )
        leaving[-1].start()
    leaving.append(pltpu.make_async_copy(o, out_ref.at[0], out_sems.at[count]))
    leaving[-1].start()
    for copy in leaving:
        copy.wait()


def unpack_kernel(home_ref, *rest, count, q_width, kv_width):
    blocks = rest[:count]
    qg_ref, kg_ref, vg_ref, pkg_ref, pvg_ref, parts, sems = rest[count:]
    rank = lax.axis_index("seq")
    prompt_rows = pkg_ref.shape[0]
    copies = []
    for distance in range(count):
        low = q_width + 2 * kv_width
        copies.append(
            pltpu.make_async_copy(
                blocks[distance].at[:, pl.ds(low, 2 * kv_width)], parts.at[distance], sems.at[distance, 0]
            )
        )
        copies[-1].start()
    moves = []
    for distance in range(count):
        index = resident_of(home_ref, rank ^ distance, count)
        low = 0
        for part, ref in enumerate((qg_ref, kg_ref, vg_ref)):
            width = ref.shape[2]
            moves.append(
                pltpu.make_async_copy(
                    blocks[distance].at[:, pl.ds(low, width)], ref.at[index], sems.at[distance, part + 1]
                )
            )
            moves[-1].start()
            low += width
    for copy in copies:
        copy.wait()
    summed = parts[0].astype(F32)
    for distance in range(1, count):
        summed += parts[distance].astype(F32)
    pkg_ref[...] = summed[:prompt_rows, :kv_width].astype(BF16)
    pvg_ref[...] = summed[:prompt_rows, kv_width:].astype(BF16)
    for copy in moves:
        copy.wait()


def exchange(blocks):
    count = len(blocks)
    return [blocks[0]] + [
        lax.ppermute(blocks[d], "seq", [(i, i ^ d) for i in range(count)]) for d in range(1, count)
    ]


ANY = pl.BlockSpec(memory_space=pl.ANY)
SMEM = pl.BlockSpec(memory_space=pltpu.SMEM)
VMEM = pl.BlockSpec(memory_space=pltpu.VMEM)


def packed_body(
    response_query,
    response_key,
    response_value,
    response_grad,
    prompt_key,
    prompt_value,
    lengths,
    home_rank,
    prompt_seen,
):
    count = home_rank.shape[0]
    rows, q_width = response_query.shape[1:]
    prompt_rows, kv_width = prompt_key.shape
    total = rows * count
    in_width = 2 * q_width + 4 * kv_width
    back_width = q_width + 4 * kv_width
    blocks = pl.pallas_call(
        functools.partial(pack_kernel, count=count),
        name="pack",
        out_shape=[jax.ShapeDtypeStruct((rows, in_width), BF16)] * count,
        in_specs=[SMEM, ANY, ANY, ANY, ANY, VMEM, VMEM],
        out_specs=[ANY] * count,
        scratch_shapes=[pltpu.VMEM((rows, 2 * kv_width), BF16), pltpu.SemaphoreType.DMA((count, 5))],
    )(home_rank, response_query, response_key, response_value, response_grad, prompt_key, prompt_value)
    arrived = exchange(blocks)
    output, *returns = pl.pallas_call(
        functools.partial(
            attend_kernel, count=count, prompt_rows=prompt_rows, q_width=q_width, kv_width=kv_width
        ),
        name="attend",
        out_shape=[jax.ShapeDtypeStruct((1, total, q_width), BF16)]
        + [jax.ShapeDtypeStruct((rows, back_width), BF16)] * count,
        in_specs=[SMEM] * 3 + [ANY] * count,
        out_specs=[ANY] * (count + 1),
        scratch_shapes=[
            pltpu.VMEM((total, in_width), BF16),
            pltpu.VMEM((total, back_width), BF16),
            pltpu.VMEM((total, q_width), BF16),
            pltpu.SemaphoreType.DMA((count,)),
            pltpu.SemaphoreType.DMA((count + 1,)),
        ],
    )(lengths, home_rank, prompt_seen, *arrived)
    returned = exchange(returns)
    grads = pl.pallas_call(
        functools.partial(unpack_kernel, count=count, q_width=q_width, kv_width=kv_width),
        name="unpack",
        out_shape=[
            jax.ShapeDtypeStruct((count, rows, q_width), BF16),
            jax.ShapeDtypeStruct((count, rows, kv_width), BF16),
            jax.ShapeDtypeStruct((count, rows, kv_width), BF16),
            jax.ShapeDtypeStruct((prompt_rows, kv_width), BF16),
            jax.ShapeDtypeStruct((prompt_rows, kv_width), BF16),
        ],
        in_specs=[SMEM] + [ANY] * count,
        out_specs=[ANY, ANY, ANY, VMEM, VMEM],
        scratch_shapes=[
            pltpu.VMEM((count, rows, 2 * kv_width), BF16),
            pltpu.SemaphoreType.DMA((count, 4)),
        ],
    )(home_rank, *returned)
    return (output, *grads)


def head_logits(queries, all_keys, allowed, head_index, group_size, scale_factor):
    row_count = queries.shape[0]
    low = head_index * group_size * HEAD_DIM
    high = (head_index + 1) * group_size * HEAD_DIM
    query_head = queries[:, low:high].reshape(row_count, group_size, HEAD_DIM)
    key_head = all_keys[:, head_index * HEAD_DIM : (head_index + 1) * HEAD_DIM]
    logits = (
        jnp.einsum("rhd,kd->rhk", query_head, key_head, preferred_element_type=jnp.float32)
        * scale_factor
    )
    return (query_head, key_head, jnp.where(allowed[:, None, :], logits, NEG_FILL))


def forward(queries, all_keys, all_values, allowed, live_rows, scale_factor):
    row_count = queries.shape[0]
    kv_count = all_keys.shape[1] // HEAD_DIM
    group_size = queries.shape[1] // all_keys.shape[1]
    outputs = []
    totals = []
    for head_index in range(kv_count):
        query_head, key_head, logits = head_logits(
            queries, all_keys, allowed, head_index, group_size, scale_factor
        )
        value_head = all_values[:, head_index * HEAD_DIM : (head_index + 1) * HEAD_DIM]
        row_max = jnp.max(logits, axis=2, keepdims=True)
        log_total = row_max + jnp.log(jnp.sum(jnp.exp(logits - row_max), axis=2, keepdims=True))
        weights = jnp.exp(logits - log_total).astype(jnp.bfloat16)
        mixed = jnp.einsum("rhk,kd->rhd", weights, value_head, preferred_element_type=jnp.float32)
        output_head = jnp.where(live_rows[:, None, None], mixed, 0.0).astype(jnp.bfloat16)
        outputs.append(output_head.reshape(row_count, group_size * HEAD_DIM))
        totals.append(log_total)
    return (jnp.concatenate(outputs, axis=1), totals)


def head_terms(grad_rows, live_rows, output, head_index, group_size):
    row_count = grad_rows.shape[0]
    low = head_index * group_size * HEAD_DIM
    high = (head_index + 1) * group_size * HEAD_DIM
    grad_head = jnp.where(live_rows[:, None], grad_rows[:, low:high], jnp.zeros((), jnp.bfloat16))
    grad_head = grad_head.reshape(row_count, group_size, HEAD_DIM)
    output_head = lax.optimization_barrier(output[:, low:high]).reshape(
        row_count, group_size, HEAD_DIM
    )
    row_dot = jnp.sum(
        grad_head.astype(jnp.float32) * output_head.astype(jnp.float32), axis=2, keepdims=True
    )
    return (grad_head, row_dot)


def backward(
    queries, all_keys, all_values, grad_rows, allowed, live_rows, output, totals, scale_factor
):
    row_count = queries.shape[0]
    kv_count = all_keys.shape[1] // HEAD_DIM
    group_size = queries.shape[1] // all_keys.shape[1]
    query_grads = []
    key_grads = []
    value_grads = []
    for head_index in range(kv_count):
        query_head, key_head, logits = head_logits(
            queries, all_keys, allowed, head_index, group_size, scale_factor
        )
        value_head = all_values[:, head_index * HEAD_DIM : (head_index + 1) * HEAD_DIM]
        prob = jnp.exp(logits - totals[head_index])
        weights = prob.astype(jnp.bfloat16)
        grad_head, row_dot = head_terms(grad_rows, live_rows, output, head_index, group_size)
        spread = jnp.einsum(
            "rhd,kd->rhk", grad_head, value_head, preferred_element_type=jnp.float32
        )
        dlogit = (prob * (spread - row_dot)).astype(jnp.bfloat16)
        query_part = (
            jnp.einsum("rhk,kd->rhd", dlogit, key_head, preferred_element_type=jnp.float32)
            * scale_factor
        )
        query_grads.append(query_part.reshape(row_count, group_size * HEAD_DIM))
        key_grads.append(
            jnp.einsum("rhk,rhd->kd", dlogit, query_head, preferred_element_type=jnp.float32)
            * scale_factor
        )
        value_grads.append(
            jnp.einsum("rhk,rhd->kd", weights, grad_head, preferred_element_type=jnp.float32)
        )
    return (
        jnp.concatenate(query_grads, axis=1),
        jnp.concatenate(key_grads, axis=1),
        jnp.concatenate(value_grads, axis=1),
    )


def body(
    response_query,
    response_key,
    response_value,
    response_grad,
    prompt_key,
    prompt_value,
    lengths,
    home_rank,
    prompt_seen,
):
    rank_count = home_rank.shape[0]
    rank_ids = jnp.arange(rank_count, dtype=jnp.int32)
    resident = jnp.sum(
        jnp.where(home_rank[None, :] == rank_ids[:, None], rank_ids[None, :], 0), axis=1
    )
    own_rank = lax.axis_index("seq")
    scale_factor = 1.0 / HEAD_DIM**0.5
    arrived = (
        lax.all_to_all(response_query[resident], "seq", split_axis=0, concat_axis=1, tiled=True),
        lax.all_to_all(response_key[resident], "seq", split_axis=0, concat_axis=1, tiled=True),
        lax.all_to_all(response_value[resident], "seq", split_axis=0, concat_axis=1, tiled=True),
        lax.all_to_all(response_grad[resident], "seq", split_axis=0, concat_axis=1, tiled=True),
    )
    queries = arrived[0][0]
    own_keys = arrived[1][0]
    own_values = arrived[2][0]
    grad_rows = arrived[3][0]
    own_response = resident[own_rank]
    length = lengths[own_response]
    visible = prompt_seen[own_response]
    max_length = queries.shape[0]
    prompt_rows = prompt_key.shape[0]
    prompt_total = prompt_rows * lax.axis_size("seq")
    positions = jnp.arange(max_length, dtype=jnp.int32)
    prompt_cols = jnp.arange(prompt_total, dtype=jnp.int32)
    seen_part = jnp.broadcast_to(prompt_cols[None, :] < visible, (max_length, prompt_total))
    allowed = jnp.concatenate([seen_part, positions[None, :] <= positions[:, None]], axis=1)
    live_rows = positions < length
    gathered_keys, gathered_values = (
        lax.all_gather(prompt_key, "seq", axis=0, tiled=True),
        lax.all_gather(prompt_value, "seq", axis=0, tiled=True),
    )
    all_keys = jnp.concatenate([gathered_keys, own_keys], axis=0)
    all_values = jnp.concatenate([gathered_values, own_values], axis=0)
    response_out, response_totals = forward(
        queries, all_keys, all_values, allowed, live_rows, scale_factor
    )
    query_grad, key_grad, value_grad = backward(
        queries,
        all_keys,
        all_values,
        grad_rows,
        allowed,
        live_rows,
        response_out,
        response_totals,
        scale_factor,
    )
    key_summed, value_summed = (
        lax.psum_scatter(key_grad[:prompt_total], "seq", scatter_dimension=0, tiled=True),
        lax.psum_scatter(value_grad[:prompt_total], "seq", scatter_dimension=0, tiled=True),
    )
    returned = (
        lax.all_to_all(
            query_grad.astype(jnp.bfloat16)[None], "seq", split_axis=1, concat_axis=0, tiled=True
        ),
        lax.all_to_all(
            key_grad[prompt_total:].astype(jnp.bfloat16)[None],
            "seq",
            split_axis=1,
            concat_axis=0,
            tiled=True,
        ),
        lax.all_to_all(
            value_grad[prompt_total:].astype(jnp.bfloat16)[None],
            "seq",
            split_axis=1,
            concat_axis=0,
            tiled=True,
        ),
    )
    return (
        response_out[None],
        returned[0][home_rank],
        returned[1][home_rank],
        returned[2][home_rank],
        key_summed.astype(jnp.bfloat16),
        value_summed.astype(jnp.bfloat16),
    )


def choose_body(response_query, *others):
    count, rows = response_query.shape[:2]
    prompt_rows = others[3].shape[0]
    fits = rows % 16 == 0 and prompt_rows <= rows and rows * count == HEAD_DIM
    if fits and count & (count - 1) == 0 and count <= 16:
        return packed_body(response_query, *others)
    return body(response_query, *others)


def solution(mesh):
    placed = (
        P("group", "seq", "head"),
        P("group", "seq", "head"),
        P("group", "seq", "head"),
        P("group", "seq", "head"),
        P(("group", "seq"), "head"),
        P(("group", "seq"), "head"),
        P("group"),
        P("group"),
        P("group"),
    )
    return jax.shard_map(
        choose_body,
        mesh=mesh,
        in_specs=placed,
        out_specs=(
            P(("group", "seq"), None, "head"),
            P("group", "seq", "head"),
            P("group", "seq", "head"),
            P("group", "seq", "head"),
            P(("group", "seq"), "head"),
            P(("group", "seq"), "head"),
        ),
        check_vma=False,
    )
```

```python
import functools

import jax
import jax.numpy as jnp
from jax import lax
from jax.experimental import pallas as pl
from jax.experimental.pallas import tpu as pltpu
from jax.sharding import PartitionSpec as P

HEAD_DIM = 128


NEG_FILL = -1e30
BF16 = jnp.bfloat16
F32 = jnp.float32


def resident_of(home_ref, rank, count):
    found = jnp.int32(0)
    for index in range(count):
        found = jnp.where(home_ref[index] == rank, jnp.int32(index), found)
    return found


def dot(left, right, contract):
    return lax.dot_general(left, right, ((contract[0], contract[1]), ((), ())), preferred_element_type=F32)


def pack_kernel(home_ref, q_ref, k_ref, v_ref, g_ref, pk_ref, pv_ref, *blocks, count):
    rank = lax.axis_index("seq")
    prompt_rows, kv_width = pk_ref.shape
    rows = q_ref.shape[1]
    spare = jnp.zeros((rows - prompt_rows, kv_width), BF16)
    prompt = [jnp.concatenate([ref[...], spare], axis=0) for ref in (pk_ref, pv_ref)]
    for distance in range(count):
        index = resident_of(home_ref, rank ^ distance, count)
        low = 0
        for ref in (q_ref, g_ref, k_ref, v_ref):
            blocks[distance][:, low : low + ref.shape[2]] = ref[index]
            low += ref.shape[2]
        for part in prompt:
            blocks[distance][:, low : low + kv_width] = part
            low += kv_width


def attend_kernel(lengths_ref, home_ref, seen_ref, *rest, count, prompt_rows, q_width, kv_width):
    blocks = rest[:count]
    out_ref = rest[count]
    returns = rest[count + 1 : 2 * count + 1]
    x, y = rest[2 * count + 1 :]
    rank = lax.axis_index("seq")
    rows = blocks[0].shape[0]
    total = rows * count
    kv_count = kv_width // HEAD_DIM
    group_size = q_width // kv_width
    scale = 1.0 / HEAD_DIM**0.5
    for distance in range(count):
        x[pl.ds(pl.multiple_of((rank ^ distance) * rows, rows), rows), :] = blocks[distance][...]
    own = resident_of(home_ref, rank, count)
    length = lengths_ref[own]
    visible = seen_ref[own]
    column = lax.broadcasted_iota(jnp.int32, (total, total), 1)
    position = lax.broadcasted_iota(jnp.int32, (total, total), 0)
    shard_row = column % rows
    prompt_index = column // rows * prompt_rows + shard_row
    allowed = jnp.concatenate(
        [(shard_row < prompt_rows) & (prompt_index < visible), column <= position], axis=1
    )
    live = lax.broadcasted_iota(jnp.int32, (total, HEAD_DIM), 0) < length
    for kv in range(kv_count):
        low = 2 * q_width + kv * HEAD_DIM
        keys = jnp.concatenate(
            [x[:, low + 2 * kv_width : low + 2 * kv_width + HEAD_DIM], x[:, low : low + HEAD_DIM]], axis=0
        )
        low += kv_width
        values = jnp.concatenate(
            [x[:, low + 2 * kv_width : low + 2 * kv_width + HEAD_DIM], x[:, low : low + HEAD_DIM]], axis=0
        )
        key_grad = jnp.zeros((2 * total, HEAD_DIM), F32)
        value_grad = jnp.zeros((2 * total, HEAD_DIM), F32)
        for member in range(group_size):
            head = (kv * group_size + member) * HEAD_DIM
            query = x[:, head : head + HEAD_DIM]
            grad = jnp.where(live, x[:, q_width + head : q_width + head + HEAD_DIM], jnp.zeros((), BF16))
            logits = jnp.where(allowed, dot(query, keys, ((1,), (1,))) * scale, NEG_FILL)
            spread = dot(grad, values, ((1,), (1,)))
            raised = jnp.exp(logits - jnp.max(logits, axis=1, keepdims=True))
            prob = raised * (1.0 / jnp.sum(raised, axis=1, keepdims=True))
            weights = prob.astype(BF16)
            output = jnp.where(live, dot(weights, values, ((1,), (0,))), 0.0).astype(BF16)
            out_ref[0, :, head : head + HEAD_DIM] = output
            row_dot = jnp.sum(grad.astype(F32) * output.astype(F32), axis=1, keepdims=True)
            dlogit = (prob * (spread - row_dot)).astype(BF16)
            y[:, head : head + HEAD_DIM] = (dot(dlogit, keys, ((1,), (0,))) * scale).astype(BF16)
            key_grad += dot(dlogit, query, ((0,), (0,)))
            value_grad += dot(weights, grad, ((0,), (0,)))
        low = q_width + kv * HEAD_DIM
        for part, summed in enumerate((key_grad * scale, value_grad)):
            at = low + part * kv_width
            y[:, at : at + HEAD_DIM] = summed[total:].astype(BF16)
            at += 2 * kv_width
            y[:, at : at + HEAD_DIM] = summed[:total].astype(BF16)
    for distance in range(count):
        returns[distance][...] = y[pl.ds(pl.multiple_of((rank ^ distance) * rows, rows), rows), :]


def unpack_kernel(home_ref, *rest, count, kv_width):
    blocks = rest[:count]
    qg_ref, kg_ref, vg_ref, pkg_ref, pvg_ref = rest[count:]
    rank = lax.axis_index("seq")
    prompt_rows = pkg_ref.shape[0]
    summed = [jnp.zeros((blocks[0].shape[0], kv_width), F32)] * 2
    for distance in range(count):
        index = resident_of(home_ref, rank ^ distance, count)
        low = 0
        for ref in (qg_ref, kg_ref, vg_ref):
            ref[index] = blocks[distance][:, low : low + ref.shape[2]]
            low += ref.shape[2]
        for part in range(2):
            summed[part] = summed[part] + blocks[distance][:, low : low + kv_width].astype(F32)
            low += kv_width
    pkg_ref[...] = summed[0][:prompt_rows].astype(BF16)
    pvg_ref[...] = summed[1][:prompt_rows].astype(BF16)


def exchange(blocks):
    count = len(blocks)
    return [blocks[0]] + [
        lax.ppermute(blocks[d], "seq", [(i, i ^ d) for i in range(count)]) for d in range(1, count)
    ]


SMEM = pl.BlockSpec(memory_space=pltpu.SMEM)
VMEM = pl.BlockSpec(memory_space=pltpu.VMEM)


def packed_body(
    response_query,
    response_key,
    response_value,
    response_grad,
    prompt_key,
    prompt_value,
    lengths,
    home_rank,
    prompt_seen,
):
    count = home_rank.shape[0]
    rows, q_width = response_query.shape[1:]
    prompt_rows, kv_width = prompt_key.shape
    total = rows * count
    in_width = 2 * q_width + 4 * kv_width
    back_width = q_width + 4 * kv_width
    blocks = pl.pallas_call(
        functools.partial(pack_kernel, count=count),
        name="pack",
        out_shape=[jax.ShapeDtypeStruct((rows, in_width), BF16)] * count,
        in_specs=[SMEM] + [VMEM] * 6,
        out_specs=[VMEM] * count,
    )(home_rank, response_query, response_key, response_value, response_grad, prompt_key, prompt_value)
    arrived = exchange(blocks)
    output, *returns = pl.pallas_call(
        functools.partial(
            attend_kernel, count=count, prompt_rows=prompt_rows, q_width=q_width, kv_width=kv_width
        ),
        name="attend",
        out_shape=[jax.ShapeDtypeStruct((1, total, q_width), BF16)]
        + [jax.ShapeDtypeStruct((rows, back_width), BF16)] * count,
        in_specs=[SMEM] * 3 + [VMEM] * count,
        out_specs=[VMEM] * (count + 1),
        scratch_shapes=[
            pltpu.VMEM((total, in_width), BF16),
            pltpu.VMEM((total, back_width), BF16),
        ],
    )(lengths, home_rank, prompt_seen, *arrived)
    returned = exchange(returns)
    grads = pl.pallas_call(
        functools.partial(unpack_kernel, count=count, kv_width=kv_width),
        name="unpack",
        out_shape=[
            jax.ShapeDtypeStruct((count, rows, q_width), BF16),
            jax.ShapeDtypeStruct((count, rows, kv_width), BF16),
            jax.ShapeDtypeStruct((count, rows, kv_width), BF16),
            jax.ShapeDtypeStruct((prompt_rows, kv_width), BF16),
            jax.ShapeDtypeStruct((prompt_rows, kv_width), BF16),
        ],
        in_specs=[SMEM] + [VMEM] * count,
        out_specs=[VMEM] * 5,
    )(home_rank, *returned)
    return (output, *grads)


def head_logits(queries, all_keys, allowed, head_index, group_size, scale_factor):
    row_count = queries.shape[0]
    low = head_index * group_size * HEAD_DIM
    high = (head_index + 1) * group_size * HEAD_DIM
    query_head = queries[:, low:high].reshape(row_count, group_size, HEAD_DIM)
    key_head = all_keys[:, head_index * HEAD_DIM : (head_index + 1) * HEAD_DIM]
    logits = (
        jnp.einsum("rhd,kd->rhk", query_head, key_head, preferred_element_type=jnp.float32)
        * scale_factor
    )
    return (query_head, key_head, jnp.where(allowed[:, None, :], logits, NEG_FILL))


def forward(queries, all_keys, all_values, allowed, live_rows, scale_factor):
    row_count = queries.shape[0]
    kv_count = all_keys.shape[1] // HEAD_DIM
    group_size = queries.shape[1] // all_keys.shape[1]
    outputs = []
    totals = []
    for head_index in range(kv_count):
        query_head, key_head, logits = head_logits(
            queries, all_keys, allowed, head_index, group_size, scale_factor
        )
        value_head = all_values[:, head_index * HEAD_DIM : (head_index + 1) * HEAD_DIM]
        row_max = jnp.max(logits, axis=2, keepdims=True)
        log_total = row_max + jnp.log(jnp.sum(jnp.exp(logits - row_max), axis=2, keepdims=True))
        weights = jnp.exp(logits - log_total).astype(jnp.bfloat16)
        mixed = jnp.einsum("rhk,kd->rhd", weights, value_head, preferred_element_type=jnp.float32)
        output_head = jnp.where(live_rows[:, None, None], mixed, 0.0).astype(jnp.bfloat16)
        outputs.append(output_head.reshape(row_count, group_size * HEAD_DIM))
        totals.append(log_total)
    return (jnp.concatenate(outputs, axis=1), totals)


def head_terms(grad_rows, live_rows, output, head_index, group_size):
    row_count = grad_rows.shape[0]
    low = head_index * group_size * HEAD_DIM
    high = (head_index + 1) * group_size * HEAD_DIM
    grad_head = jnp.where(live_rows[:, None], grad_rows[:, low:high], jnp.zeros((), jnp.bfloat16))
    grad_head = grad_head.reshape(row_count, group_size, HEAD_DIM)
    output_head = lax.optimization_barrier(output[:, low:high]).reshape(
        row_count, group_size, HEAD_DIM
    )
    row_dot = jnp.sum(
        grad_head.astype(jnp.float32) * output_head.astype(jnp.float32), axis=2, keepdims=True
    )
    return (grad_head, row_dot)


def backward(
    queries, all_keys, all_values, grad_rows, allowed, live_rows, output, totals, scale_factor
):
    row_count = queries.shape[0]
    kv_count = all_keys.shape[1] // HEAD_DIM
    group_size = queries.shape[1] // all_keys.shape[1]
    query_grads = []
    key_grads = []
    value_grads = []
    for head_index in range(kv_count):
        query_head, key_head, logits = head_logits(
            queries, all_keys, allowed, head_index, group_size, scale_factor
        )
        value_head = all_values[:, head_index * HEAD_DIM : (head_index + 1) * HEAD_DIM]
        prob = jnp.exp(logits - totals[head_index])
        weights = prob.astype(jnp.bfloat16)
        grad_head, row_dot = head_terms(grad_rows, live_rows, output, head_index, group_size)
        spread = jnp.einsum(
            "rhd,kd->rhk", grad_head, value_head, preferred_element_type=jnp.float32
        )
        dlogit = (prob * (spread - row_dot)).astype(jnp.bfloat16)
        query_part = (
            jnp.einsum("rhk,kd->rhd", dlogit, key_head, preferred_element_type=jnp.float32)
            * scale_factor
        )
        query_grads.append(query_part.reshape(row_count, group_size * HEAD_DIM))
        key_grads.append(
            jnp.einsum("rhk,rhd->kd", dlogit, query_head, preferred_element_type=jnp.float32)
            * scale_factor
        )
        value_grads.append(
            jnp.einsum("rhk,rhd->kd", weights, grad_head, preferred_element_type=jnp.float32)
        )
    return (
        jnp.concatenate(query_grads, axis=1),
        jnp.concatenate(key_grads, axis=1),
        jnp.concatenate(value_grads, axis=1),
    )


def body(
    response_query,
    response_key,
    response_value,
    response_grad,
    prompt_key,
    prompt_value,
    lengths,
    home_rank,
    prompt_seen,
):
    rank_count = home_rank.shape[0]
    rank_ids = jnp.arange(rank_count, dtype=jnp.int32)
    resident = jnp.sum(
        jnp.where(home_rank[None, :] == rank_ids[:, None], rank_ids[None, :], 0), axis=1
    )
    own_rank = lax.axis_index("seq")
    scale_factor = 1.0 / HEAD_DIM**0.5
    arrived = (
        lax.all_to_all(response_query[resident], "seq", split_axis=0, concat_axis=1, tiled=True),
        lax.all_to_all(response_key[resident], "seq", split_axis=0, concat_axis=1, tiled=True),
        lax.all_to_all(response_value[resident], "seq", split_axis=0, concat_axis=1, tiled=True),
        lax.all_to_all(response_grad[resident], "seq", split_axis=0, concat_axis=1, tiled=True),
    )
    queries = arrived[0][0]
    own_keys = arrived[1][0]
    own_values = arrived[2][0]
    grad_rows = arrived[3][0]
    own_response = resident[own_rank]
    length = lengths[own_response]
    visible = prompt_seen[own_response]
    max_length = queries.shape[0]
    prompt_rows = prompt_key.shape[0]
    prompt_total = prompt_rows * lax.axis_size("seq")
    positions = jnp.arange(max_length, dtype=jnp.int32)
    prompt_cols = jnp.arange(prompt_total, dtype=jnp.int32)
    seen_part = jnp.broadcast_to(prompt_cols[None, :] < visible, (max_length, prompt_total))
    allowed = jnp.concatenate([seen_part, positions[None, :] <= positions[:, None]], axis=1)
    live_rows = positions < length
    gathered_keys, gathered_values = (
        lax.all_gather(prompt_key, "seq", axis=0, tiled=True),
        lax.all_gather(prompt_value, "seq", axis=0, tiled=True),
    )
    all_keys = jnp.concatenate([gathered_keys, own_keys], axis=0)
    all_values = jnp.concatenate([gathered_values, own_values], axis=0)
    response_out, response_totals = forward(
        queries, all_keys, all_values, allowed, live_rows, scale_factor
    )
    query_grad, key_grad, value_grad = backward(
        queries,
        all_keys,
        all_values,
        grad_rows,
        allowed,
        live_rows,
        response_out,
        response_totals,
        scale_factor,
    )
    key_summed, value_summed = (
        lax.psum_scatter(key_grad[:prompt_total], "seq", scatter_dimension=0, tiled=True),
        lax.psum_scatter(value_grad[:prompt_total], "seq", scatter_dimension=0, tiled=True),
    )
    returned = (
        lax.all_to_all(
            query_grad.astype(jnp.bfloat16)[None], "seq", split_axis=1, concat_axis=0, tiled=True
        ),
        lax.all_to_all(
            key_grad[prompt_total:].astype(jnp.bfloat16)[None],
            "seq",
            split_axis=1,
            concat_axis=0,
            tiled=True,
        ),
        lax.all_to_all(
            value_grad[prompt_total:].astype(jnp.bfloat16)[None],
            "seq",
            split_axis=1,
            concat_axis=0,
            tiled=True,
        ),
    )
    return (
        response_out[None],
        returned[0][home_rank],
        returned[1][home_rank],
        returned[2][home_rank],
        key_summed.astype(jnp.bfloat16),
        value_summed.astype(jnp.bfloat16),
    )


def choose_body(response_query, *others):
    count, rows = response_query.shape[:2]
    prompt_rows = others[3].shape[0]
    fits = rows % 16 == 0 and prompt_rows <= rows and rows * count == HEAD_DIM
    if fits and count & (count - 1) == 0 and count <= 16:
        return packed_body(response_query, *others)
    return body(response_query, *others)


def solution(mesh):
    placed = (
        P("group", "seq", "head"),
        P("group", "seq", "head"),
        P("group", "seq", "head"),
        P("group", "seq", "head"),
        P(("group", "seq"), "head"),
        P(("group", "seq"), "head"),
        P("group"),
        P("group"),
        P("group"),
    )
    return jax.shard_map(
        choose_body,
        mesh=mesh,
        in_specs=placed,
        out_specs=(
            P(("group", "seq"), None, "head"),
            P("group", "seq", "head"),
            P("group", "seq", "head"),
            P("group", "seq", "head"),
            P(("group", "seq"), "head"),
            P(("group", "seq"), "head"),
        ),
        check_vma=False,
    )
```

```python
import functools

import jax
import jax.numpy as jnp
from jax import lax
from jax.experimental import pallas as pl
from jax.experimental.pallas import tpu as pltpu
from jax.sharding import PartitionSpec as P

HEAD_DIM = 128


NEG_FILL = -1e30
BF16 = jnp.bfloat16
F32 = jnp.float32


def resident_of(home_ref, rank, count):
    found = jnp.int32(0)
    for index in range(count):
        found = jnp.where(home_ref[index] == rank, jnp.int32(index), found)
    return found


def dot(left, right, contract):
    return lax.dot_general(left, right, ((contract[0], contract[1]), ((), ())), preferred_element_type=F32)


def pack_kernel(home_ref, q_ref, k_ref, v_ref, g_ref, pk_ref, pv_ref, *blocks, count, heads):
    rank = lax.axis_index("seq")
    prompt_rows = pk_ref.shape[0]
    rows = q_ref.shape[1]
    near = count // 2
    q_part = q_ref.shape[2] // heads
    spare = jnp.zeros((rows - prompt_rows, HEAD_DIM), BF16)
    width = 2 * q_part + 4 * HEAD_DIM
    for head in range(heads):
        lanes = slice(head * HEAD_DIM, (head + 1) * HEAD_DIM)
        wide = slice(head * q_part, (head + 1) * q_part)
        prompt = [jnp.concatenate([ref[:, lanes], spare], axis=0) for ref in (pk_ref, pv_ref)]
        for distance in [*range(near, count), *range(near)]:
            index = resident_of(home_ref, rank ^ distance, count)
            if distance < near:
                block, low = blocks[distance], head * width
            else:
                block, low = blocks[near + head * (count - near) + distance - near], 0
            for ref, part in ((q_ref, wide), (g_ref, wide), (k_ref, lanes), (v_ref, lanes)):
                size = part.stop - part.start
                block[:, low : low + size] = ref[index, :, part]
                low += size
            for rows_of in prompt:
                block[:, low : low + HEAD_DIM] = rows_of
                low += HEAD_DIM


def attend_kernel(lengths_ref, home_ref, seen_ref, *rest, count, prompt_rows, head, heads):
    near = count // 2
    last = head == heads - 1
    blocks, rest = rest[:count], rest[count:]
    kept, rest = rest[: (head if last else 0) * (near + 1)], rest[(head if last else 0) * (near + 1) :]
    out_ref, returns, (x, y) = rest[0], rest[1 : count + 1], rest[count + 1 :]
    rank = lax.axis_index("seq")
    rows, width = blocks[near].shape
    total = rows * count
    q_part = (width - 4 * HEAD_DIM) // 2
    back = q_part + 4 * HEAD_DIM
    scale = 1.0 / HEAD_DIM**0.5
    for distance in range(count):
        low = head * width if distance < near else 0
        at = pl.ds(pl.multiple_of((rank ^ distance) * rows, rows), rows)
        x[at, :] = blocks[distance][:, low : low + width]
    own = resident_of(home_ref, rank, count)
    length = lengths_ref[own]
    visible = seen_ref[own]
    column = lax.broadcasted_iota(jnp.int32, (total, total), 1)
    position = lax.broadcasted_iota(jnp.int32, (total, total), 0)
    shard_row = column % rows
    prompt_index = column // rows * prompt_rows + shard_row
    allowed = jnp.concatenate(
        [(shard_row < prompt_rows) & (prompt_index < visible), column <= position], axis=1
    )
    live = lax.broadcasted_iota(jnp.int32, (total, HEAD_DIM), 0) < length
    out_low = head * q_part if last else 0

    def lanes(low):
        return x[:, low : low + HEAD_DIM]

    low = 2 * q_part
    keys = jnp.concatenate([lanes(low + 2 * HEAD_DIM), lanes(low)], axis=0)
    values = jnp.concatenate([lanes(low + 3 * HEAD_DIM), lanes(low + HEAD_DIM)], axis=0)
    key_grad = jnp.zeros((2 * total, HEAD_DIM), F32)
    value_grad = jnp.zeros((2 * total, HEAD_DIM), F32)
    for low in range(0, q_part, HEAD_DIM):
        query = lanes(low)
        grad = jnp.where(live, lanes(q_part + low), jnp.zeros((), BF16))
        logits = jnp.where(allowed, dot(query, keys, ((1,), (1,))) * scale, NEG_FILL)
        spread = dot(grad, values, ((1,), (1,)))
        raised = jnp.exp(logits - jnp.max(logits, axis=1, keepdims=True))
        prob = raised * (1.0 / jnp.sum(raised, axis=1, keepdims=True))
        weights = prob.astype(BF16)
        output = jnp.where(live, dot(weights, values, ((1,), (0,))), 0.0).astype(BF16)
        out_ref[0, :, out_low + low : out_low + low + HEAD_DIM] = output
        row_dot = jnp.sum(grad.astype(F32) * output.astype(F32), axis=1, keepdims=True)
        dlogit = (prob * (spread - row_dot)).astype(BF16)
        y[:, low : low + HEAD_DIM] = (dot(dlogit, keys, ((1,), (0,))) * scale).astype(BF16)
        key_grad += dot(dlogit, query, ((0,), (0,)))
        value_grad += dot(weights, grad, ((0,), (0,)))
    for part, summed in enumerate((key_grad * scale, value_grad)):
        at = q_part + part * HEAD_DIM
        y[:, at : at + HEAD_DIM] = summed[total:].astype(BF16)
        at += 2 * HEAD_DIM
        y[:, at : at + HEAD_DIM] = summed[:total].astype(BF16)
    for distance in range(count):
        low = head * back if last and distance < near else 0
        at = pl.ds(pl.multiple_of((rank ^ distance) * rows, rows), rows)
        returns[distance][:, low : low + back] = y[at, :]
    for earlier in range(len(kept) // (near + 1)):
        parts = kept[earlier * (near + 1) : (earlier + 1) * (near + 1)]
        out_ref[0, :, earlier * q_part : (earlier + 1) * q_part] = parts[0][0]
        for distance in range(near):
            returns[distance][:, earlier * back : (earlier + 1) * back] = parts[1 + distance][...]


def unpack_kernel(home_ref, *rest, count, heads):
    near = count // 2
    blocks = rest[:-5]
    qg_ref, kg_ref, vg_ref, pkg_ref, pvg_ref = rest[-5:]
    rank = lax.axis_index("seq")
    prompt_rows = pkg_ref.shape[0]
    q_part = qg_ref.shape[2] // heads
    back = q_part + 4 * HEAD_DIM
    for head in range(heads):
        lanes = slice(head * HEAD_DIM, (head + 1) * HEAD_DIM)
        wide = slice(head * q_part, (head + 1) * q_part)
        summed = [jnp.zeros((qg_ref.shape[1], HEAD_DIM), F32)] * 2
        for distance in range(count):
            index = resident_of(home_ref, rank ^ distance, count)
            if distance < near:
                block, low = blocks[distance], head * back
            else:
                block, low = blocks[near + head * (count - near) + distance - near], 0
            for ref, part in ((qg_ref, wide), (kg_ref, lanes), (vg_ref, lanes)):
                size = part.stop - part.start
                ref[index, :, part] = block[:, low : low + size]
                low += size
            for part in range(2):
                summed[part] = summed[part] + block[:, low : low + HEAD_DIM].astype(F32)
                low += HEAD_DIM
        pkg_ref[:, lanes] = summed[0][:prompt_rows].astype(BF16)
        pvg_ref[:, lanes] = summed[1][:prompt_rows].astype(BF16)


def exchange(blocks, distances, count):
    arrived = []
    for block, distance in zip(blocks, distances):
        if distance:
            block = lax.ppermute(block, "seq", [(i, i ^ distance) for i in range(count)])
        arrived.append(block)
    return arrived


SMEM = pl.BlockSpec(memory_space=pltpu.SMEM)
VMEM = pl.BlockSpec(memory_space=pltpu.VMEM)
PARAMS = pltpu.CompilerParams(vmem_limit_bytes=24 * 1024 * 1024)


def packed_body(
    response_query,
    response_key,
    response_value,
    response_grad,
    prompt_key,
    prompt_value,
    lengths,
    home_rank,
    prompt_seen,
):
    count = home_rank.shape[0]
    rows, q_width = response_query.shape[1:]
    prompt_rows, kv_width = prompt_key.shape
    total = rows * count
    heads = kv_width // HEAD_DIM
    near, far = range(count // 2), range(count // 2, count)
    q_part = q_width // heads
    width = 2 * q_part + 4 * HEAD_DIM
    back = q_part + 4 * HEAD_DIM

    def shape(*dims):
        return jax.ShapeDtypeStruct(dims, BF16)

    packed = pl.pallas_call(
        functools.partial(pack_kernel, count=count, heads=heads),
        name="pack",
        out_shape=[shape(rows, heads * width)] * len(near) + [shape(rows, width)] * (len(far) * heads),
        in_specs=[SMEM] + [VMEM] * 6,
        out_specs=[VMEM] * (len(near) + len(far) * heads),
        compiler_params=PARAMS,
    )(home_rank, response_query, response_key, response_value, response_grad, prompt_key, prompt_value)
    far_in = [exchange(packed[len(near) :][: len(far)], far, count)]
    near_in = exchange(packed[: len(near)], near, count)
    for head in range(1, heads):
        blocks = packed[len(near) + head * len(far) :][: len(far)]
        far_in.append(exchange(blocks, far, count))
    kept, far_back = [], []
    for head in range(heads):
        last = head == heads - 1
        whole = heads if last else 1
        operands = [lengths, home_rank, prompt_seen, *near_in, *far_in[head], *(kept if last else [])]
        results = pl.pallas_call(
            functools.partial(
                attend_kernel, count=count, prompt_rows=prompt_rows, head=head, heads=heads
            ),
            out_shape=[shape(1, total, whole * q_part)]
            + [shape(rows, whole * back)] * len(near)
            + [shape(rows, back)] * len(far),
            in_specs=[SMEM] * 3 + [VMEM] * (len(operands) - 3),
            out_specs=[VMEM] * (count + 1),
            scratch_shapes=[pltpu.VMEM((total, width), BF16), pltpu.VMEM((total, back), BF16)],
            compiler_params=PARAMS,
        )(*operands)
        far_back += exchange(results[1 + len(near) :], far, count)
        kept += results[: 1 + len(near)]
    output, *near_back = kept[-1 - len(near) :]
    near_back = exchange(near_back, near, count)
    grads = pl.pallas_call(
        functools.partial(unpack_kernel, count=count, heads=heads),
        name="unpack",
        out_shape=[
            shape(count, rows, q_width),
            shape(count, rows, kv_width),
            shape(count, rows, kv_width),
            shape(prompt_rows, kv_width),
            shape(prompt_rows, kv_width),
        ],
        in_specs=[SMEM] + [VMEM] * (len(near) + len(far) * heads),
        out_specs=[VMEM] * 5,
        compiler_params=PARAMS,
    )(home_rank, *near_back, *far_back)
    return (output, *grads)


def head_logits(queries, all_keys, allowed, head_index, group_size, scale_factor):
    row_count = queries.shape[0]
    low = head_index * group_size * HEAD_DIM
    high = (head_index + 1) * group_size * HEAD_DIM
    query_head = queries[:, low:high].reshape(row_count, group_size, HEAD_DIM)
    key_head = all_keys[:, head_index * HEAD_DIM : (head_index + 1) * HEAD_DIM]
    logits = (
        jnp.einsum("rhd,kd->rhk", query_head, key_head, preferred_element_type=jnp.float32)
        * scale_factor
    )
    return (query_head, key_head, jnp.where(allowed[:, None, :], logits, NEG_FILL))


def forward(queries, all_keys, all_values, allowed, live_rows, scale_factor):
    row_count = queries.shape[0]
    kv_count = all_keys.shape[1] // HEAD_DIM
    group_size = queries.shape[1] // all_keys.shape[1]
    outputs = []
    totals = []
    for head_index in range(kv_count):
        _, _, logits = head_logits(
            queries, all_keys, allowed, head_index, group_size, scale_factor
        )
        value_head = all_values[:, head_index * HEAD_DIM : (head_index + 1) * HEAD_DIM]
        row_max = jnp.max(logits, axis=2, keepdims=True)
        log_total = row_max + jnp.log(jnp.sum(jnp.exp(logits - row_max), axis=2, keepdims=True))
        weights = jnp.exp(logits - log_total).astype(jnp.bfloat16)
        mixed = jnp.einsum("rhk,kd->rhd", weights, value_head, preferred_element_type=jnp.float32)
        output_head = jnp.where(live_rows[:, None, None], mixed, 0.0).astype(jnp.bfloat16)
        outputs.append(output_head.reshape(row_count, group_size * HEAD_DIM))
        totals.append(log_total)
    return (jnp.concatenate(outputs, axis=1), totals)


def head_terms(grad_rows, live_rows, output, head_index, group_size):
    row_count = grad_rows.shape[0]
    low = head_index * group_size * HEAD_DIM
    high = (head_index + 1) * group_size * HEAD_DIM
    grad_head = jnp.where(live_rows[:, None], grad_rows[:, low:high], jnp.zeros((), jnp.bfloat16))
    grad_head = grad_head.reshape(row_count, group_size, HEAD_DIM)
    output_head = lax.optimization_barrier(output[:, low:high]).reshape(
        row_count, group_size, HEAD_DIM
    )
    row_dot = jnp.sum(
        grad_head.astype(jnp.float32) * output_head.astype(jnp.float32), axis=2, keepdims=True
    )
    return (grad_head, row_dot)


def backward(
    queries, all_keys, all_values, grad_rows, allowed, live_rows, output, totals, scale_factor
):
    row_count = queries.shape[0]
    kv_count = all_keys.shape[1] // HEAD_DIM
    group_size = queries.shape[1] // all_keys.shape[1]
    query_grads = []
    key_grads = []
    value_grads = []
    for head_index in range(kv_count):
        query_head, key_head, logits = head_logits(
            queries, all_keys, allowed, head_index, group_size, scale_factor
        )
        value_head = all_values[:, head_index * HEAD_DIM : (head_index + 1) * HEAD_DIM]
        prob = jnp.exp(logits - totals[head_index])
        weights = prob.astype(jnp.bfloat16)
        grad_head, row_dot = head_terms(grad_rows, live_rows, output, head_index, group_size)
        spread = jnp.einsum(
            "rhd,kd->rhk", grad_head, value_head, preferred_element_type=jnp.float32
        )
        dlogit = (prob * (spread - row_dot)).astype(jnp.bfloat16)
        query_part = (
            jnp.einsum("rhk,kd->rhd", dlogit, key_head, preferred_element_type=jnp.float32)
            * scale_factor
        )
        query_grads.append(query_part.reshape(row_count, group_size * HEAD_DIM))
        key_grads.append(
            jnp.einsum("rhk,rhd->kd", dlogit, query_head, preferred_element_type=jnp.float32)
            * scale_factor
        )
        value_grads.append(
            jnp.einsum("rhk,rhd->kd", weights, grad_head, preferred_element_type=jnp.float32)
        )
    return (
        jnp.concatenate(query_grads, axis=1),
        jnp.concatenate(key_grads, axis=1),
        jnp.concatenate(value_grads, axis=1),
    )


def body(
    response_query,
    response_key,
    response_value,
    response_grad,
    prompt_key,
    prompt_value,
    lengths,
    home_rank,
    prompt_seen,
):
    rank_count = home_rank.shape[0]
    rank_ids = jnp.arange(rank_count, dtype=jnp.int32)
    resident = jnp.sum(
        jnp.where(home_rank[None, :] == rank_ids[:, None], rank_ids[None, :], 0), axis=1
    )
    own_rank = lax.axis_index("seq")
    scale_factor = 1.0 / HEAD_DIM**0.5
    arrived = (
        lax.all_to_all(response_query[resident], "seq", split_axis=0, concat_axis=1, tiled=True),
        lax.all_to_all(response_key[resident], "seq", split_axis=0, concat_axis=1, tiled=True),
        lax.all_to_all(response_value[resident], "seq", split_axis=0, concat_axis=1, tiled=True),
        lax.all_to_all(response_grad[resident], "seq", split_axis=0, concat_axis=1, tiled=True),
    )
    queries = arrived[0][0]
    own_keys = arrived[1][0]
    own_values = arrived[2][0]
    grad_rows = arrived[3][0]
    own_response = resident[own_rank]
    length = lengths[own_response]
    visible = prompt_seen[own_response]
    max_length = queries.shape[0]
    prompt_rows = prompt_key.shape[0]
    prompt_total = prompt_rows * lax.axis_size("seq")
    positions = jnp.arange(max_length, dtype=jnp.int32)
    prompt_cols = jnp.arange(prompt_total, dtype=jnp.int32)
    seen_part = jnp.broadcast_to(prompt_cols[None, :] < visible, (max_length, prompt_total))
    allowed = jnp.concatenate([seen_part, positions[None, :] <= positions[:, None]], axis=1)
    live_rows = positions < length
    gathered_keys, gathered_values = (
        lax.all_gather(prompt_key, "seq", axis=0, tiled=True),
        lax.all_gather(prompt_value, "seq", axis=0, tiled=True),
    )
    all_keys = jnp.concatenate([gathered_keys, own_keys], axis=0)
    all_values = jnp.concatenate([gathered_values, own_values], axis=0)
    response_out, response_totals = forward(
        queries, all_keys, all_values, allowed, live_rows, scale_factor
    )
    query_grad, key_grad, value_grad = backward(
        queries,
        all_keys,
        all_values,
        grad_rows,
        allowed,
        live_rows,
        response_out,
        response_totals,
        scale_factor,
    )
    key_summed, value_summed = (
        lax.psum_scatter(key_grad[:prompt_total], "seq", scatter_dimension=0, tiled=True),
        lax.psum_scatter(value_grad[:prompt_total], "seq", scatter_dimension=0, tiled=True),
    )
    returned = (
        lax.all_to_all(
            query_grad.astype(jnp.bfloat16)[None], "seq", split_axis=1, concat_axis=0, tiled=True
        ),
        lax.all_to_all(
            key_grad[prompt_total:].astype(jnp.bfloat16)[None],
            "seq",
            split_axis=1,
            concat_axis=0,
            tiled=True,
        ),
        lax.all_to_all(
            value_grad[prompt_total:].astype(jnp.bfloat16)[None],
            "seq",
            split_axis=1,
            concat_axis=0,
            tiled=True,
        ),
    )
    return (
        response_out[None],
        returned[0][home_rank],
        returned[1][home_rank],
        returned[2][home_rank],
        key_summed.astype(jnp.bfloat16),
        value_summed.astype(jnp.bfloat16),
    )


def choose_body(response_query, *others):
    count, rows = response_query.shape[:2]
    prompt_rows = others[3].shape[0]
    fits = rows % 16 == 0 and prompt_rows <= rows and rows * count == HEAD_DIM
    if fits and count & (count - 1) == 0 and count <= 16:
        return packed_body(response_query, *others)
    return body(response_query, *others)


def solution(mesh):
    placed = (
        P("group", "seq", "head"),
        P("group", "seq", "head"),
        P("group", "seq", "head"),
        P("group", "seq", "head"),
        P(("group", "seq"), "head"),
        P(("group", "seq"), "head"),
        P("group"),
        P("group"),
        P("group"),
    )
    return jax.shard_map(
        choose_body,
        mesh=mesh,
        in_specs=placed,
        out_specs=(
            P(("group", "seq"), None, "head"),
            P("group", "seq", "head"),
            P("group", "seq", "head"),
            P("group", "seq", "head"),
            P(("group", "seq"), "head"),
            P(("group", "seq"), "head"),
        ),
        check_vma=False,
    )
```

```python
import functools

import jax
import jax.numpy as jnp
from jax import lax
from jax.experimental import pallas as pl
from jax.experimental.pallas import tpu as pltpu
from jax.sharding import PartitionSpec as P

HEAD_DIM = 128


NEG_FILL = -1e30
BF16 = jnp.bfloat16
F32 = jnp.float32


def resident_of(home_ref, rank, count):
    found = jnp.int32(0)
    for index in range(count):
        found = jnp.where(home_ref[index] == rank, jnp.int32(index), found)
    return found


def dot(left, right, contract):
    return lax.dot_general(left, right, ((contract[0], contract[1]), ((), ())), preferred_element_type=F32)


def pack_kernel(home_ref, q_ref, k_ref, v_ref, g_ref, pk_ref, pv_ref, *rest, count, head, heads, by_rank):
    blocks, (home, q, g, k, v, prompt, sems) = rest[:-7], rest[-7:]
    rank = lax.axis_index("seq")
    prompt_rows = pk_ref.shape[0]
    q_part = q.shape[2]
    lanes = pl.ds(head * HEAD_DIM, HEAD_DIM)
    wide = pl.ds(head * q_part, q_part)
    copies = [
        pltpu.make_async_copy(source, target, sems.at[index])
        for index, (source, target) in enumerate(
            (
                (home_ref, home),
                (q_ref.at[:, :, wide], q),
                (g_ref.at[:, :, wide], g),
                (k_ref.at[:, :, lanes], k),
                (v_ref.at[:, :, lanes], v),
                (pk_ref.at[:, lanes], prompt.at[0]),
                (pv_ref.at[:, lanes], prompt.at[1]),
            )
        )
    ]
    for copy in copies:
        copy.start()
    for copy in copies:
        copy.wait()
    rows = q.shape[1]
    spare = jnp.zeros((rows - prompt_rows, HEAD_DIM), BF16)
    padded = [jnp.concatenate([prompt[part], spare], axis=0) for part in range(2)]
    for place in range(count):
        index = resident_of(home, place if by_rank else rank ^ place, count)
        block = blocks[0].at[place] if by_rank else blocks[place]
        low = 0
        for ref in (q, g, k, v):
            block[:, low : low + ref.shape[2]] = ref[index]
            low += ref.shape[2]
        for part in padded:
            block[:, low : low + HEAD_DIM] = part
            low += HEAD_DIM


def attend_kernel(lengths_ref, home_ref, seen_ref, *rest, count, prompt_rows, by_rank):
    blocks, rest = (rest[:1], rest[1:]) if by_rank else (rest[:count], rest[count:])
    if by_rank:
        (out_ref, y) = rest
        x = blocks[0]
        rows, width = x.shape[1:]
    else:
        earlier_ref, out_ref, *returns, x, y = rest
        rows, width = blocks[0].shape
    total = rows * count
    q_part = (width - 4 * HEAD_DIM) // 2
    scale = 1.0 / HEAD_DIM**0.5
    rank = lax.axis_index("seq")
    out_low = 0
    if not by_rank:
        for distance in range(count):
            x[rank ^ distance] = blocks[distance][...]
        out_low = earlier_ref.shape[2]
        out_ref[:, :, :out_low] = earlier_ref[...]
    own = resident_of(home_ref, rank, count)
    length = lengths_ref[own]
    visible = seen_ref[own]
    column = lax.broadcasted_iota(jnp.int32, (total, total), 1)
    position = lax.broadcasted_iota(jnp.int32, (total, total), 0)
    shard_row = column % rows
    prompt_index = column // rows * prompt_rows + shard_row
    allowed = jnp.concatenate(
        [(shard_row < prompt_rows) & (prompt_index < visible), column <= position], axis=1
    )
    live = lax.broadcasted_iota(jnp.int32, (total, HEAD_DIM), 0) < length

    def lanes(low):
        return x[:, :, low : low + HEAD_DIM].reshape(total, HEAD_DIM)

    def give(low, value):
        y[:, :, low : low + HEAD_DIM] = value.astype(BF16).reshape(count, rows, HEAD_DIM)

    low = 2 * q_part
    keys = jnp.concatenate([lanes(low + 2 * HEAD_DIM), lanes(low)], axis=0)
    values = jnp.concatenate([lanes(low + 3 * HEAD_DIM), lanes(low + HEAD_DIM)], axis=0)
    key_grad = jnp.zeros((2 * total, HEAD_DIM), F32)
    value_grad = jnp.zeros((2 * total, HEAD_DIM), F32)
    for low in range(0, q_part, HEAD_DIM):
        query = lanes(low)
        grad = jnp.where(live, lanes(q_part + low), jnp.zeros((), BF16))
        logits = jnp.where(allowed, dot(query, keys, ((1,), (1,))) * scale, NEG_FILL)
        spread = dot(grad, values, ((1,), (1,)))
        raised = jnp.exp(logits - jnp.max(logits, axis=1, keepdims=True))
        prob = raised * (1.0 / jnp.sum(raised, axis=1, keepdims=True))
        weights = prob.astype(BF16)
        output = jnp.where(live, dot(weights, values, ((1,), (0,))), 0.0).astype(BF16)
        out_ref[0, :, out_low + low : out_low + low + HEAD_DIM] = output
        row_dot = jnp.sum(grad.astype(F32) * output.astype(F32), axis=1, keepdims=True)
        dlogit = (prob * (spread - row_dot)).astype(BF16)
        give(low, dot(dlogit, keys, ((1,), (0,))) * scale)
        key_grad += dot(dlogit, query, ((0,), (0,)))
        value_grad += dot(weights, grad, ((0,), (0,)))
    for part, summed in enumerate((key_grad * scale, value_grad)):
        give(q_part + part * HEAD_DIM, summed[total:])
        give(q_part + (part + 2) * HEAD_DIM, summed[:total])
    if not by_rank:
        for distance in range(count):
            returns[distance][...] = y[rank ^ distance]


def unpack_kernel(home_ref, *rest, count, heads):
    blocks = rest[:-5]
    qg_ref, kg_ref, vg_ref, pkg_ref, pvg_ref = rest[-5:]
    rank = lax.axis_index("seq")
    prompt_rows = pkg_ref.shape[0]
    q_part = qg_ref.shape[2] // heads
    for head in range(heads):
        lanes = slice(head * HEAD_DIM, (head + 1) * HEAD_DIM)
        wide = slice(head * q_part, (head + 1) * q_part)
        summed = [jnp.zeros((qg_ref.shape[1], HEAD_DIM), F32)] * 2
        for place in range(count):
            index = resident_of(home_ref, rank ^ place if head else place, count)
            block = blocks[1 + (head - 1) * count + place] if head else blocks[0].at[place]
            low = 0
            for ref, part in ((qg_ref, wide), (kg_ref, lanes), (vg_ref, lanes)):
                size = part.stop - part.start
                ref[index, :, part] = block[:, low : low + size]
                low += size
            for part in range(2):
                summed[part] = summed[part] + block[:, low : low + HEAD_DIM].astype(F32)
                low += HEAD_DIM
        pkg_ref[:, lanes] = summed[0][:prompt_rows].astype(BF16)
        pvg_ref[:, lanes] = summed[1][:prompt_rows].astype(BF16)


def exchange(blocks):
    count = len(blocks)
    arrived = list(blocks)
    for distance in range(1, count):
        arrived[distance] = lax.ppermute(
            blocks[distance], "seq", [(i, i ^ distance) for i in range(count)]
        )
    return arrived


def exchange_by_rank(blocks):
    return lax.all_to_all(blocks, "seq", split_axis=0, concat_axis=0, tiled=True)


SMEM = pl.BlockSpec(memory_space=pltpu.SMEM)
VMEM = pl.BlockSpec(memory_space=pltpu.VMEM)
HBM = pl.BlockSpec(memory_space=pltpu.HBM)
PARAMS = pltpu.CompilerParams(vmem_limit_bytes=24 * 1024 * 1024)


def packed_body(
    response_query,
    response_key,
    response_value,
    response_grad,
    prompt_key,
    prompt_value,
    lengths,
    home_rank,
    prompt_seen,
):
    count = home_rank.shape[0]
    rows, q_width = response_query.shape[1:]
    prompt_rows, kv_width = prompt_key.shape
    total = rows * count
    heads = kv_width // HEAD_DIM
    q_part = q_width // heads
    width = 2 * q_part + 4 * HEAD_DIM
    back = q_part + 4 * HEAD_DIM

    def shapes(by_rank, lanes):
        dims = [(count, rows, lanes)] if by_rank else [(rows, lanes)] * count
        return [jax.ShapeDtypeStruct(each, BF16) for each in dims]

    arrived = []
    sources = [
        pltpu.with_memory_space_constraint(source, pltpu.HBM)
        for source in (home_rank, response_query, response_key, response_value, response_grad, prompt_key, prompt_value)
    ]
    for head in range(heads):
        by_rank = head == 0
        results = shapes(by_rank, width)
        blocks = pl.pallas_call(
            functools.partial(pack_kernel, count=count, head=head, heads=heads, by_rank=by_rank),
            out_shape=results,
            in_specs=[HBM] * 7,
            out_specs=[VMEM] * len(results),
            scratch_shapes=[pltpu.SMEM((count,), jnp.int32)]
            + [pltpu.VMEM((count, rows, lanes), BF16) for lanes in (q_part, q_part, HEAD_DIM, HEAD_DIM)]
            + [pltpu.VMEM((2, prompt_rows, HEAD_DIM), BF16), pltpu.SemaphoreType.DMA((7,))],
            compiler_params=PARAMS,
        )(*sources)
        arrived.append([exchange_by_rank(blocks[0])] if by_rank else exchange(blocks))
    output, returned = [], []
    for head in range(heads):
        by_rank = head == 0
        operands = [lengths, home_rank, prompt_seen, *arrived[head], *output]
        results = [jax.ShapeDtypeStruct((1, total, (head + 1) * q_part), BF16)] + shapes(by_rank, back)
        scratch = [] if by_rank else [pltpu.VMEM((count, rows, lanes), BF16) for lanes in (width, back)]
        output, *blocks = pl.pallas_call(
            functools.partial(attend_kernel, count=count, prompt_rows=prompt_rows, by_rank=by_rank),
            out_shape=results,
            in_specs=[SMEM] * 3 + [VMEM] * (len(operands) - 3),
            out_specs=[VMEM] * len(results),
            scratch_shapes=scratch,
            compiler_params=PARAMS,
        )(*operands)
        output = [output]
        returned += [exchange_by_rank(blocks[0])] if by_rank else exchange(blocks)
    grads = pl.pallas_call(
        functools.partial(unpack_kernel, count=count, heads=heads),
        name="unpack",
        out_shape=[
            jax.ShapeDtypeStruct(dims, BF16)
            for dims in ((count, rows, q_width), *[(count, rows, kv_width)] * 2, *[(prompt_rows, kv_width)] * 2)
        ],
        in_specs=[SMEM] + [VMEM] * len(returned),
        out_specs=[VMEM] * 5,
        compiler_params=PARAMS,
    )(home_rank, *returned)
    return (output[0], *grads)


def head_logits(queries, all_keys, allowed, head_index, group_size, scale_factor):
    row_count = queries.shape[0]
    low = head_index * group_size * HEAD_DIM
    high = (head_index + 1) * group_size * HEAD_DIM
    query_head = queries[:, low:high].reshape(row_count, group_size, HEAD_DIM)
    key_head = all_keys[:, head_index * HEAD_DIM : (head_index + 1) * HEAD_DIM]
    logits = (
        jnp.einsum("rhd,kd->rhk", query_head, key_head, preferred_element_type=jnp.float32)
        * scale_factor
    )
    return (query_head, key_head, jnp.where(allowed[:, None, :], logits, NEG_FILL))


def forward(queries, all_keys, all_values, allowed, live_rows, scale_factor):
    row_count = queries.shape[0]
    kv_count = all_keys.shape[1] // HEAD_DIM
    group_size = queries.shape[1] // all_keys.shape[1]
    outputs = []
    totals = []
    for head_index in range(kv_count):
        _, _, logits = head_logits(
            queries, all_keys, allowed, head_index, group_size, scale_factor
        )
        value_head = all_values[:, head_index * HEAD_DIM : (head_index + 1) * HEAD_DIM]
        row_max = jnp.max(logits, axis=2, keepdims=True)
        log_total = row_max + jnp.log(jnp.sum(jnp.exp(logits - row_max), axis=2, keepdims=True))
        weights = jnp.exp(logits - log_total).astype(jnp.bfloat16)
        mixed = jnp.einsum("rhk,kd->rhd", weights, value_head, preferred_element_type=jnp.float32)
        output_head = jnp.where(live_rows[:, None, None], mixed, 0.0).astype(jnp.bfloat16)
        outputs.append(output_head.reshape(row_count, group_size * HEAD_DIM))
        totals.append(log_total)
    return (jnp.concatenate(outputs, axis=1), totals)


def head_terms(grad_rows, live_rows, output, head_index, group_size):
    row_count = grad_rows.shape[0]
    low = head_index * group_size * HEAD_DIM
    high = (head_index + 1) * group_size * HEAD_DIM
    grad_head = jnp.where(live_rows[:, None], grad_rows[:, low:high], jnp.zeros((), jnp.bfloat16))
    grad_head = grad_head.reshape(row_count, group_size, HEAD_DIM)
    output_head = lax.optimization_barrier(output[:, low:high]).reshape(
        row_count, group_size, HEAD_DIM
    )
    row_dot = jnp.sum(
        grad_head.astype(jnp.float32) * output_head.astype(jnp.float32), axis=2, keepdims=True
    )
    return (grad_head, row_dot)


def backward(
    queries, all_keys, all_values, grad_rows, allowed, live_rows, output, totals, scale_factor
):
    row_count = queries.shape[0]
    kv_count = all_keys.shape[1] // HEAD_DIM
    group_size = queries.shape[1] // all_keys.shape[1]
    query_grads = []
    key_grads = []
    value_grads = []
    for head_index in range(kv_count):
        query_head, key_head, logits = head_logits(
            queries, all_keys, allowed, head_index, group_size, scale_factor
        )
        value_head = all_values[:, head_index * HEAD_DIM : (head_index + 1) * HEAD_DIM]
        prob = jnp.exp(logits - totals[head_index])
        weights = prob.astype(jnp.bfloat16)
        grad_head, row_dot = head_terms(grad_rows, live_rows, output, head_index, group_size)
        spread = jnp.einsum(
            "rhd,kd->rhk", grad_head, value_head, preferred_element_type=jnp.float32
        )
        dlogit = (prob * (spread - row_dot)).astype(jnp.bfloat16)
        query_part = (
            jnp.einsum("rhk,kd->rhd", dlogit, key_head, preferred_element_type=jnp.float32)
            * scale_factor
        )
        query_grads.append(query_part.reshape(row_count, group_size * HEAD_DIM))
        key_grads.append(
            jnp.einsum("rhk,rhd->kd", dlogit, query_head, preferred_element_type=jnp.float32)
            * scale_factor
        )
        value_grads.append(
            jnp.einsum("rhk,rhd->kd", weights, grad_head, preferred_element_type=jnp.float32)
        )
    return (
        jnp.concatenate(query_grads, axis=1),
        jnp.concatenate(key_grads, axis=1),
        jnp.concatenate(value_grads, axis=1),
    )


def body(
    response_query,
    response_key,
    response_value,
    response_grad,
    prompt_key,
    prompt_value,
    lengths,
    home_rank,
    prompt_seen,
):
    rank_count = home_rank.shape[0]
    rank_ids = jnp.arange(rank_count, dtype=jnp.int32)
    resident = jnp.sum(
        jnp.where(home_rank[None, :] == rank_ids[:, None], rank_ids[None, :], 0), axis=1
    )
    own_rank = lax.axis_index("seq")
    scale_factor = 1.0 / HEAD_DIM**0.5
    arrived = (
        lax.all_to_all(response_query[resident], "seq", split_axis=0, concat_axis=1, tiled=True),
        lax.all_to_all(response_key[resident], "seq", split_axis=0, concat_axis=1, tiled=True),
        lax.all_to_all(response_value[resident], "seq", split_axis=0, concat_axis=1, tiled=True),
        lax.all_to_all(response_grad[resident], "seq", split_axis=0, concat_axis=1, tiled=True),
    )
    queries = arrived[0][0]
    own_keys = arrived[1][0]
    own_values = arrived[2][0]
    grad_rows = arrived[3][0]
    own_response = resident[own_rank]
    length = lengths[own_response]
    visible = prompt_seen[own_response]
    max_length = queries.shape[0]
    prompt_rows = prompt_key.shape[0]
    prompt_total = prompt_rows * lax.axis_size("seq")
    positions = jnp.arange(max_length, dtype=jnp.int32)
    prompt_cols = jnp.arange(prompt_total, dtype=jnp.int32)
    seen_part = jnp.broadcast_to(prompt_cols[None, :] < visible, (max_length, prompt_total))
    allowed = jnp.concatenate([seen_part, positions[None, :] <= positions[:, None]], axis=1)
    live_rows = positions < length
    gathered_keys, gathered_values = (
        lax.all_gather(prompt_key, "seq", axis=0, tiled=True),
        lax.all_gather(prompt_value, "seq", axis=0, tiled=True),
    )
    all_keys = jnp.concatenate([gathered_keys, own_keys], axis=0)
    all_values = jnp.concatenate([gathered_values, own_values], axis=0)
    response_out, response_totals = forward(
        queries, all_keys, all_values, allowed, live_rows, scale_factor
    )
    query_grad, key_grad, value_grad = backward(
        queries,
        all_keys,
        all_values,
        grad_rows,
        allowed,
        live_rows,
        response_out,
        response_totals,
        scale_factor,
    )
    key_summed, value_summed = (
        lax.psum_scatter(key_grad[:prompt_total], "seq", scatter_dimension=0, tiled=True),
        lax.psum_scatter(value_grad[:prompt_total], "seq", scatter_dimension=0, tiled=True),
    )
    returned = (
        lax.all_to_all(
            query_grad.astype(jnp.bfloat16)[None], "seq", split_axis=1, concat_axis=0, tiled=True
        ),
        lax.all_to_all(
            key_grad[prompt_total:].astype(jnp.bfloat16)[None],
            "seq",
            split_axis=1,
            concat_axis=0,
            tiled=True,
        ),
        lax.all_to_all(
            value_grad[prompt_total:].astype(jnp.bfloat16)[None],
            "seq",
            split_axis=1,
            concat_axis=0,
            tiled=True,
        ),
    )
    return (
        response_out[None],
        returned[0][home_rank],
        returned[1][home_rank],
        returned[2][home_rank],
        key_summed.astype(jnp.bfloat16),
        value_summed.astype(jnp.bfloat16),
    )


def choose_body(response_query, *others):
    count, rows = response_query.shape[:2]
    prompt_rows = others[3].shape[0]
    fits = rows % 16 == 0 and prompt_rows <= rows and rows * count == HEAD_DIM
    if fits and count & (count - 1) == 0 and count <= 16:
        return packed_body(response_query, *others)
    return body(response_query, *others)


def solution(mesh):
    placed = (
        P("group", "seq", "head"),
        P("group", "seq", "head"),
        P("group", "seq", "head"),
        P("group", "seq", "head"),
        P(("group", "seq"), "head"),
        P(("group", "seq"), "head"),
        P("group"),
        P("group"),
        P("group"),
    )
    return jax.shard_map(
        choose_body,
        mesh=mesh,
        in_specs=placed,
        out_specs=(
            P(("group", "seq"), None, "head"),
            P("group", "seq", "head"),
            P("group", "seq", "head"),
            P("group", "seq", "head"),
            P(("group", "seq"), "head"),
            P(("group", "seq"), "head"),
        ),
        check_vma=False,
    )
```

```python
import functools

import jax
import jax.numpy as jnp
from jax import lax
from jax.experimental import pallas as pl
from jax.experimental.pallas import tpu as pltpu
from jax.sharding import PartitionSpec as P

HEAD_DIM = 128


NEG_FILL = -1e30
BF16 = jnp.bfloat16
F32 = jnp.float32


def resident_of(home_ref, rank, count):
    found = jnp.int32(0)
    for index in range(count):
        found = jnp.where(home_ref[index] == rank, jnp.int32(index), found)
    return found


def dot(left, right, contract):
    return lax.dot_general(left, right, ((contract[0], contract[1]), ((), ())), preferred_element_type=F32)


def pack_kernel(home_ref, q_ref, k_ref, v_ref, g_ref, pk_ref, pv_ref, *rest, count, head, heads, by_rank):
    blocks, (home, q, g, k, v, prompt, sems) = rest[:-7], rest[-7:]
    rank = lax.axis_index("seq")
    prompt_rows = pk_ref.shape[0]
    q_part = q.shape[2]
    lanes = pl.ds(head * HEAD_DIM, HEAD_DIM)
    wide = pl.ds(head * q_part, q_part)
    copies = [
        pltpu.make_async_copy(source, target, sems.at[index])
        for index, (source, target) in enumerate(
            (
                (home_ref, home),
                (q_ref.at[:, :, wide], q),
                (g_ref.at[:, :, wide], g),
                (k_ref.at[:, :, lanes], k),
                (v_ref.at[:, :, lanes], v),
                (pk_ref.at[:, lanes], prompt.at[0]),
                (pv_ref.at[:, lanes], prompt.at[1]),
            )
        )
    ]
    for copy in copies:
        copy.start()
    for copy in copies:
        copy.wait()
    rows = q.shape[1]
    spare = jnp.zeros((rows - prompt_rows, HEAD_DIM), BF16)
    padded = [jnp.concatenate([prompt[part], spare], axis=0) for part in range(2)]
    for place in range(count):
        index = resident_of(home, place if by_rank else rank ^ place, count)
        block = blocks[0].at[place] if by_rank else blocks[place]
        low = 0
        for ref in (q, g, k, v):
            block[:, low : low + ref.shape[2]] = ref[index]
            low += ref.shape[2]
        for part in padded:
            block[:, low : low + HEAD_DIM] = part
            low += HEAD_DIM


def attend_kernel(lengths_ref, home_ref, seen_ref, *rest, count, prompt_rows, head, heads):
    near = count // 2
    by_rank = head > 0
    last = head == heads - 1
    taken = 1 if by_rank else count
    blocks, rest = rest[:taken], rest[taken:]
    kept, rest = (rest[: head * (near + 1)], rest[head * (near + 1) :]) if last else ((), rest)
    out_ref, returns, scratch = rest[0], rest[1 : count + 1], rest[count + 1 :]
    rank = lax.axis_index("seq")
    if by_rank:
        x, y = blocks[0], scratch[0]
    else:
        x, y = scratch
        for distance in range(count):
            x[rank ^ distance] = blocks[distance][...]
    rows, width = x.shape[1:]
    total = rows * count
    q_part = (width - 4 * HEAD_DIM) // 2
    scale = 1.0 / HEAD_DIM**0.5
    out_low = head * q_part if last else 0
    own = resident_of(home_ref, rank, count)
    length = lengths_ref[own]
    visible = seen_ref[own]
    column = lax.broadcasted_iota(jnp.int32, (total, total), 1)
    position = lax.broadcasted_iota(jnp.int32, (total, total), 0)
    shard_row = column % rows
    prompt_index = column // rows * prompt_rows + shard_row
    allowed = jnp.concatenate(
        [(shard_row < prompt_rows) & (prompt_index < visible), column <= position], axis=1
    )
    live = lax.broadcasted_iota(jnp.int32, (total, HEAD_DIM), 0) < length

    def lanes(low):
        return x[:, :, low : low + HEAD_DIM].reshape(total, HEAD_DIM)

    def give(low, value):
        y[:, :, low : low + HEAD_DIM] = value.astype(BF16).reshape(count, rows, HEAD_DIM)

    low = 2 * q_part
    keys = jnp.concatenate([lanes(low + 2 * HEAD_DIM), lanes(low)], axis=0)
    values = jnp.concatenate([lanes(low + 3 * HEAD_DIM), lanes(low + HEAD_DIM)], axis=0)
    key_grad = jnp.zeros((2 * total, HEAD_DIM), F32)
    value_grad = jnp.zeros((2 * total, HEAD_DIM), F32)
    for low in range(0, q_part, HEAD_DIM):
        query = lanes(low)
        grad = jnp.where(live, lanes(q_part + low), jnp.zeros((), BF16))
        logits = jnp.where(allowed, dot(query, keys, ((1,), (1,))) * scale, NEG_FILL)
        spread = dot(grad, values, ((1,), (1,)))
        raised = jnp.exp(logits - jnp.max(logits, axis=1, keepdims=True))
        prob = raised * (1.0 / jnp.sum(raised, axis=1, keepdims=True))
        weights = prob.astype(BF16)
        output = jnp.where(live, dot(weights, values, ((1,), (0,))), 0.0).astype(BF16)
        out_ref[0, :, out_low + low : out_low + low + HEAD_DIM] = output
        row_dot = jnp.sum(grad.astype(F32) * output.astype(F32), axis=1, keepdims=True)
        dlogit = (prob * (spread - row_dot)).astype(BF16)
        give(low, dot(dlogit, keys, ((1,), (0,))) * scale)
        key_grad += dot(dlogit, query, ((0,), (0,)))
        value_grad += dot(weights, grad, ((0,), (0,)))
    for part, summed in enumerate((key_grad * scale, value_grad)):
        give(q_part + part * HEAD_DIM, summed[total:])
        give(q_part + (part + 2) * HEAD_DIM, summed[:total])
    back = y.shape[2]
    for distance in range(count):
        low = head * back if last and distance < near else 0
        returns[distance][:, low : low + back] = y[rank ^ distance]
    for earlier in range(len(kept) // (near + 1)):
        parts = kept[earlier * (near + 1) : (earlier + 1) * (near + 1)]
        out_ref[:, :, earlier * q_part : (earlier + 1) * q_part] = parts[0][...]
        for distance in range(near):
            returns[distance][:, earlier * back : (earlier + 1) * back] = parts[1 + distance][...]


def unpack_kernel(home_ref, *rest, count, heads):
    near = count // 2
    blocks = rest[:-5]
    qg_ref, kg_ref, vg_ref, pkg_ref, pvg_ref = rest[-5:]
    rank = lax.axis_index("seq")
    prompt_rows = pkg_ref.shape[0]
    q_part = qg_ref.shape[2] // heads
    back = q_part + 4 * HEAD_DIM
    for head in range(heads):
        lanes = slice(head * HEAD_DIM, (head + 1) * HEAD_DIM)
        wide = slice(head * q_part, (head + 1) * q_part)
        summed = [jnp.zeros((qg_ref.shape[1], HEAD_DIM), F32)] * 2
        for distance in range(count):
            index = resident_of(home_ref, rank ^ distance, count)
            if distance < near:
                block, low = blocks[distance], head * back
            else:
                block, low = blocks[near + head * (count - near) + distance - near], 0
            for ref, part in ((qg_ref, wide), (kg_ref, lanes), (vg_ref, lanes)):
                size = part.stop - part.start
                ref[index, :, part] = block[:, low : low + size]
                low += size
            for part in range(2):
                summed[part] = summed[part] + block[:, low : low + HEAD_DIM].astype(F32)
                low += HEAD_DIM
        pkg_ref[:, lanes] = summed[0][:prompt_rows].astype(BF16)
        pvg_ref[:, lanes] = summed[1][:prompt_rows].astype(BF16)


def exchange(blocks, distances, count):
    arrived = []
    for block, distance in zip(blocks, distances):
        if distance:
            block = lax.ppermute(block, "seq", [(i, i ^ distance) for i in range(count)])
        arrived.append(block)
    return arrived


def exchange_by_rank(blocks):
    return lax.all_to_all(blocks, "seq", split_axis=0, concat_axis=0, tiled=True)


SMEM = pl.BlockSpec(memory_space=pltpu.SMEM)
VMEM = pl.BlockSpec(memory_space=pltpu.VMEM)
HBM = pl.BlockSpec(memory_space=pltpu.HBM)
PARAMS = pltpu.CompilerParams(vmem_limit_bytes=24 * 1024 * 1024)


def packed_body(
    response_query,
    response_key,
    response_value,
    response_grad,
    prompt_key,
    prompt_value,
    lengths,
    home_rank,
    prompt_seen,
):
    count = home_rank.shape[0]
    rows, q_width = response_query.shape[1:]
    prompt_rows, kv_width = prompt_key.shape
    total = rows * count
    heads = kv_width // HEAD_DIM
    q_part = q_width // heads
    width = 2 * q_part + 4 * HEAD_DIM
    back = q_part + 4 * HEAD_DIM

    def shapes(by_rank, lanes):
        dims = [(count, rows, lanes)] if by_rank else [(rows, lanes)] * count
        return [jax.ShapeDtypeStruct(each, BF16) for each in dims]

    arrived = []
    sources = [
        pltpu.with_memory_space_constraint(source, pltpu.HBM)
        for source in (home_rank, response_query, response_key, response_value, response_grad, prompt_key, prompt_value)
    ]
    for head in range(heads):
        by_rank = head > 0
        results = shapes(by_rank, width)
        blocks = pl.pallas_call(
            functools.partial(pack_kernel, count=count, head=head, heads=heads, by_rank=by_rank),
            out_shape=results,
            in_specs=[HBM] * 7,
            out_specs=[VMEM] * len(results),
            scratch_shapes=[pltpu.SMEM((count,), jnp.int32)]
            + [pltpu.VMEM((count, rows, lanes), BF16) for lanes in (q_part, q_part, HEAD_DIM, HEAD_DIM)]
            + [pltpu.VMEM((2, prompt_rows, HEAD_DIM), BF16), pltpu.SemaphoreType.DMA((7,))],
            compiler_params=PARAMS,
        )(*sources)
        if by_rank:
            arrived.append([exchange_by_rank(blocks[0])])
        else:
            arrived.append(exchange(blocks, range(count), count))
    near, far = range(count // 2), range(count // 2, count)
    kept, far_back = [], []
    for head in range(heads):
        last = head == heads - 1
        operands = [lengths, home_rank, prompt_seen, *arrived[head], *(kept if last else [])]
        whole = heads if last else 1
        results = [(1, total, whole * q_part)] + [(rows, whole * back)] * len(near) + [(rows, back)] * len(far)
        scratch = [back] if head else [width, back]
        results = pl.pallas_call(
            functools.partial(
                attend_kernel, count=count, prompt_rows=prompt_rows, head=head, heads=heads
            ),
            out_shape=[jax.ShapeDtypeStruct(dims, BF16) for dims in results],
            in_specs=[SMEM] * 3 + [VMEM] * (len(operands) - 3),
            out_specs=[VMEM] * len(results),
            scratch_shapes=[pltpu.VMEM((count, rows, lanes), BF16) for lanes in scratch],
            compiler_params=PARAMS,
        )(*operands)
        kept += results[: 1 + len(near)]
        far_back += exchange(results[1 + len(near) :], far, count)
    output, *near_back = kept[-1 - len(near) :]
    returned = exchange(near_back, near, count) + far_back
    grads = pl.pallas_call(
        functools.partial(unpack_kernel, count=count, heads=heads),
        name="unpack",
        out_shape=[
            jax.ShapeDtypeStruct(dims, BF16)
            for dims in ((count, rows, q_width), *[(count, rows, kv_width)] * 2, *[(prompt_rows, kv_width)] * 2)
        ],
        in_specs=[SMEM] + [VMEM] * len(returned),
        out_specs=[VMEM] * 5,
        compiler_params=PARAMS,
    )(home_rank, *returned)
    return (output, *grads)


def head_logits(queries, all_keys, allowed, head_index, group_size, scale_factor):
    row_count = queries.shape[0]
    low = head_index * group_size * HEAD_DIM
    high = (head_index + 1) * group_size * HEAD_DIM
    query_head = queries[:, low:high].reshape(row_count, group_size, HEAD_DIM)
    key_head = all_keys[:, head_index * HEAD_DIM : (head_index + 1) * HEAD_DIM]
    logits = (
        jnp.einsum("rhd,kd->rhk", query_head, key_head, preferred_element_type=jnp.float32)
        * scale_factor
    )
    return (query_head, key_head, jnp.where(allowed[:, None, :], logits, NEG_FILL))


def forward(queries, all_keys, all_values, allowed, live_rows, scale_factor):
    row_count = queries.shape[0]
    kv_count = all_keys.shape[1] // HEAD_DIM
    group_size = queries.shape[1] // all_keys.shape[1]
    outputs = []
    totals = []
    for head_index in range(kv_count):
        _, _, logits = head_logits(
            queries, all_keys, allowed, head_index, group_size, scale_factor
        )
        value_head = all_values[:, head_index * HEAD_DIM : (head_index + 1) * HEAD_DIM]
        row_max = jnp.max(logits, axis=2, keepdims=True)
        log_total = row_max + jnp.log(jnp.sum(jnp.exp(logits - row_max), axis=2, keepdims=True))
        weights = jnp.exp(logits - log_total).astype(jnp.bfloat16)
        mixed = jnp.einsum("rhk,kd->rhd", weights, value_head, preferred_element_type=jnp.float32)
        output_head = jnp.where(live_rows[:, None, None], mixed, 0.0).astype(jnp.bfloat16)
        outputs.append(output_head.reshape(row_count, group_size * HEAD_DIM))
        totals.append(log_total)
    return (jnp.concatenate(outputs, axis=1), totals)


def head_terms(grad_rows, live_rows, output, head_index, group_size):
    row_count = grad_rows.shape[0]
    low = head_index * group_size * HEAD_DIM
    high = (head_index + 1) * group_size * HEAD_DIM
    grad_head = jnp.where(live_rows[:, None], grad_rows[:, low:high], jnp.zeros((), jnp.bfloat16))
    grad_head = grad_head.reshape(row_count, group_size, HEAD_DIM)
    output_head = lax.optimization_barrier(output[:, low:high]).reshape(
        row_count, group_size, HEAD_DIM
    )
    row_dot = jnp.sum(
        grad_head.astype(jnp.float32) * output_head.astype(jnp.float32), axis=2, keepdims=True
    )
    return (grad_head, row_dot)


def backward(
    queries, all_keys, all_values, grad_rows, allowed, live_rows, output, totals, scale_factor
):
    row_count = queries.shape[0]
    kv_count = all_keys.shape[1] // HEAD_DIM
    group_size = queries.shape[1] // all_keys.shape[1]
    query_grads = []
    key_grads = []
    value_grads = []
    for head_index in range(kv_count):
        query_head, key_head, logits = head_logits(
            queries, all_keys, allowed, head_index, group_size, scale_factor
        )
        value_head = all_values[:, head_index * HEAD_DIM : (head_index + 1) * HEAD_DIM]
        prob = jnp.exp(logits - totals[head_index])
        weights = prob.astype(jnp.bfloat16)
        grad_head, row_dot = head_terms(grad_rows, live_rows, output, head_index, group_size)
        spread = jnp.einsum(
            "rhd,kd->rhk", grad_head, value_head, preferred_element_type=jnp.float32
        )
        dlogit = (prob * (spread - row_dot)).astype(jnp.bfloat16)
        query_part = (
            jnp.einsum("rhk,kd->rhd", dlogit, key_head, preferred_element_type=jnp.float32)
            * scale_factor
        )
        query_grads.append(query_part.reshape(row_count, group_size * HEAD_DIM))
        key_grads.append(
            jnp.einsum("rhk,rhd->kd", dlogit, query_head, preferred_element_type=jnp.float32)
            * scale_factor
        )
        value_grads.append(
            jnp.einsum("rhk,rhd->kd", weights, grad_head, preferred_element_type=jnp.float32)
        )
    return (
        jnp.concatenate(query_grads, axis=1),
        jnp.concatenate(key_grads, axis=1),
        jnp.concatenate(value_grads, axis=1),
    )


def body(
    response_query,
    response_key,
    response_value,
    response_grad,
    prompt_key,
    prompt_value,
    lengths,
    home_rank,
    prompt_seen,
):
    rank_count = home_rank.shape[0]
    rank_ids = jnp.arange(rank_count, dtype=jnp.int32)
    resident = jnp.sum(
        jnp.where(home_rank[None, :] == rank_ids[:, None], rank_ids[None, :], 0), axis=1
    )
    own_rank = lax.axis_index("seq")
    scale_factor = 1.0 / HEAD_DIM**0.5
    arrived = (
        lax.all_to_all(response_query[resident], "seq", split_axis=0, concat_axis=1, tiled=True),
        lax.all_to_all(response_key[resident], "seq", split_axis=0, concat_axis=1, tiled=True),
        lax.all_to_all(response_value[resident], "seq", split_axis=0, concat_axis=1, tiled=True),
        lax.all_to_all(response_grad[resident], "seq", split_axis=0, concat_axis=1, tiled=True),
    )
    queries = arrived[0][0]
    own_keys = arrived[1][0]
    own_values = arrived[2][0]
    grad_rows = arrived[3][0]
    own_response = resident[own_rank]
    length = lengths[own_response]
    visible = prompt_seen[own_response]
    max_length = queries.shape[0]
    prompt_rows = prompt_key.shape[0]
    prompt_total = prompt_rows * lax.axis_size("seq")
    positions = jnp.arange(max_length, dtype=jnp.int32)
    prompt_cols = jnp.arange(prompt_total, dtype=jnp.int32)
    seen_part = jnp.broadcast_to(prompt_cols[None, :] < visible, (max_length, prompt_total))
    allowed = jnp.concatenate([seen_part, positions[None, :] <= positions[:, None]], axis=1)
    live_rows = positions < length
    gathered_keys, gathered_values = (
        lax.all_gather(prompt_key, "seq", axis=0, tiled=True),
        lax.all_gather(prompt_value, "seq", axis=0, tiled=True),
    )
    all_keys = jnp.concatenate([gathered_keys, own_keys], axis=0)
    all_values = jnp.concatenate([gathered_values, own_values], axis=0)
    response_out, response_totals = forward(
        queries, all_keys, all_values, allowed, live_rows, scale_factor
    )
    query_grad, key_grad, value_grad = backward(
        queries,
        all_keys,
        all_values,
        grad_rows,
        allowed,
        live_rows,
        response_out,
        response_totals,
        scale_factor,
    )
    key_summed, value_summed = (
        lax.psum_scatter(key_grad[:prompt_total], "seq", scatter_dimension=0, tiled=True),
        lax.psum_scatter(value_grad[:prompt_total], "seq", scatter_dimension=0, tiled=True),
    )
    returned = (
        lax.all_to_all(
            query_grad.astype(jnp.bfloat16)[None], "seq", split_axis=1, concat_axis=0, tiled=True
        ),
        lax.all_to_all(
            key_grad[prompt_total:].astype(jnp.bfloat16)[None],
            "seq",
            split_axis=1,
            concat_axis=0,
            tiled=True,
        ),
        lax.all_to_all(
            value_grad[prompt_total:].astype(jnp.bfloat16)[None],
            "seq",
            split_axis=1,
            concat_axis=0,
            tiled=True,
        ),
    )
    return (
        response_out[None],
        returned[0][home_rank],
        returned[1][home_rank],
        returned[2][home_rank],
        key_summed.astype(jnp.bfloat16),
        value_summed.astype(jnp.bfloat16),
    )


def choose_body(response_query, *others):
    count, rows = response_query.shape[:2]
    prompt_rows = others[3].shape[0]
    fits = rows % 16 == 0 and prompt_rows <= rows and rows * count == HEAD_DIM
    if fits and count & (count - 1) == 0 and count <= 16:
        return packed_body(response_query, *others)
    return body(response_query, *others)


def solution(mesh):
    placed = (
        P("group", "seq", "head"),
        P("group", "seq", "head"),
        P("group", "seq", "head"),
        P("group", "seq", "head"),
        P(("group", "seq"), "head"),
        P(("group", "seq"), "head"),
        P("group"),
        P("group"),
        P("group"),
    )
    return jax.shard_map(
        choose_body,
        mesh=mesh,
        in_specs=placed,
        out_specs=(
            P(("group", "seq"), None, "head"),
            P("group", "seq", "head"),
            P("group", "seq", "head"),
            P("group", "seq", "head"),
            P(("group", "seq"), "head"),
            P(("group", "seq"), "head"),
        ),
        check_vma=False,
    )
```

```python
import functools

import jax
import jax.numpy as jnp
from jax import lax
from jax.experimental import pallas as pl
from jax.experimental.pallas import tpu as pltpu
from jax.sharding import PartitionSpec as P

HEAD_DIM = 128


NEG_FILL = -1e30
BF16 = jnp.bfloat16
F32 = jnp.float32


def resident_of(home_ref, rank, count):
    found = jnp.int32(0)
    for index in range(count):
        found = jnp.where(home_ref[index] == rank, jnp.int32(index), found)
    return found


def dot(left, right, contract):
    return lax.dot_general(left, right, ((contract[0], contract[1]), ((), ())), preferred_element_type=F32)


def pack_kernel(home_ref, q_ref, k_ref, v_ref, g_ref, pk_ref, pv_ref, *rest, count, head, heads, by_rank):
    blocks, (home, q, g, k, v, prompt, sems) = rest[:-7], rest[-7:]
    rank = lax.axis_index("seq")
    prompt_rows = pk_ref.shape[0]
    q_part = q.shape[2]
    lanes = pl.ds(head * HEAD_DIM, HEAD_DIM)
    wide = pl.ds(head * q_part, q_part)
    copies = [
        pltpu.make_async_copy(source, target, sems.at[index])
        for index, (source, target) in enumerate(
            (
                (home_ref, home),
                (q_ref.at[:, :, wide], q),
                (g_ref.at[:, :, wide], g),
                (k_ref.at[:, :, lanes], k),
                (v_ref.at[:, :, lanes], v),
                (pk_ref.at[:, lanes], prompt.at[0]),
                (pv_ref.at[:, lanes], prompt.at[1]),
            )
        )
    ]
    for copy in copies:
        copy.start()
    for copy in copies:
        copy.wait()
    rows = q.shape[1]
    spare = jnp.zeros((rows - prompt_rows, HEAD_DIM), BF16)
    padded = [jnp.concatenate([prompt[part], spare], axis=0) for part in range(2)]
    for place in range(count):
        index = resident_of(home, place if by_rank else rank ^ place, count)
        block = blocks[0].at[place] if by_rank else blocks[place]
        low = 0
        for ref in (q, g, k, v):
            block[:, low : low + ref.shape[2]] = ref[index]
            low += ref.shape[2]
        for part in padded:
            block[:, low : low + HEAD_DIM] = part
            low += HEAD_DIM


def attend_kernel(lengths_ref, home_ref, seen_ref, *rest, count, prompt_rows, head, heads):
    by_rank = head > 0
    last = head == heads - 1
    taken = 1 if by_rank else count
    blocks, rest = rest[:taken], rest[taken:]
    kept, rest = (rest[:head], rest[head:]) if last else ((), rest)
    out_ref, returns, scratch = rest[0], rest[1 : count + 1], rest[count + 1 :]
    rank = lax.axis_index("seq")
    if by_rank:
        x, y = blocks[0], scratch[0]
    else:
        x, y = scratch
        for distance in range(count):
            x[rank ^ distance] = blocks[distance][...]
    rows, width = x.shape[1:]
    total = rows * count
    q_part = (width - 4 * HEAD_DIM) // 2
    scale = 1.0 / HEAD_DIM**0.5
    out_low = head * q_part if last else 0
    own = resident_of(home_ref, rank, count)
    length = lengths_ref[own]
    visible = seen_ref[own]
    column = lax.broadcasted_iota(jnp.int32, (total, total), 1)
    position = lax.broadcasted_iota(jnp.int32, (total, total), 0)
    shard_row = column % rows
    prompt_index = column // rows * prompt_rows + shard_row
    allowed = jnp.concatenate(
        [(shard_row < prompt_rows) & (prompt_index < visible), column <= position], axis=1
    )
    live = lax.broadcasted_iota(jnp.int32, (total, HEAD_DIM), 0) < length

    def lanes(low):
        return x[:, :, low : low + HEAD_DIM].reshape(total, HEAD_DIM)

    def give(low, value):
        y[:, :, low : low + HEAD_DIM] = value.astype(BF16).reshape(count, rows, HEAD_DIM)

    low = 2 * q_part
    keys = jnp.concatenate([lanes(low + 2 * HEAD_DIM), lanes(low)], axis=0)
    values = jnp.concatenate([lanes(low + 3 * HEAD_DIM), lanes(low + HEAD_DIM)], axis=0)
    key_grad = jnp.zeros((2 * total, HEAD_DIM), F32)
    value_grad = jnp.zeros((2 * total, HEAD_DIM), F32)
    together = q_part // HEAD_DIM
    allowed = jnp.concatenate([allowed] * together, axis=0)
    live = jnp.concatenate([live] * together, axis=0)
    for first in range(0, q_part, together * HEAD_DIM):
        lows = range(first, min(q_part, first + together * HEAD_DIM), HEAD_DIM)
        query = jnp.concatenate([lanes(low) for low in lows], axis=0)
        grad = jnp.concatenate([lanes(q_part + low) for low in lows], axis=0)
        grad = jnp.where(live, grad, jnp.zeros((), BF16))
        logits = jnp.where(allowed, dot(query, keys, ((1,), (1,))) * scale, NEG_FILL)
        spread = dot(grad, values, ((1,), (1,)))
        raised = jnp.exp(logits - jnp.max(logits, axis=1, keepdims=True))
        prob = raised * (1.0 / jnp.sum(raised, axis=1, keepdims=True))
        weights = prob.astype(BF16)
        output = jnp.where(live, dot(weights, values, ((1,), (0,))), 0.0).astype(BF16)
        row_dot = jnp.sum(grad.astype(F32) * output.astype(F32), axis=1, keepdims=True)
        dlogit = (prob * (spread - row_dot)).astype(BF16)
        query_grad = dot(dlogit, keys, ((1,), (0,))) * scale
        for member, low in enumerate(lows):
            at = slice(member * total, (member + 1) * total)
            out_ref[0, :, out_low + low : out_low + low + HEAD_DIM] = output[at]
            give(low, query_grad[at])
        key_grad += dot(dlogit, query, ((0,), (0,)))
        value_grad += dot(weights, grad, ((0,), (0,)))
    for part, summed in enumerate((key_grad * scale, value_grad)):
        give(q_part + part * HEAD_DIM, summed[total:])
        give(q_part + (part + 2) * HEAD_DIM, summed[:total])
    for distance in range(count):
        returns[distance][...] = y[rank ^ distance]
    for earlier, part in enumerate(kept):
        out_ref[:, :, earlier * q_part : (earlier + 1) * q_part] = part[...]


def unpack_kernel(home_ref, *rest, count, heads):
    blocks = rest[:-5]
    qg_ref, kg_ref, vg_ref, pkg_ref, pvg_ref = rest[-5:]
    rank = lax.axis_index("seq")
    prompt_rows = pkg_ref.shape[0]
    q_part = qg_ref.shape[2] // heads
    for head in range(heads):
        lanes = slice(head * HEAD_DIM, (head + 1) * HEAD_DIM)
        wide = slice(head * q_part, (head + 1) * q_part)
        summed = [jnp.zeros((qg_ref.shape[1], HEAD_DIM), F32)] * 2
        for distance in range(count):
            index = resident_of(home_ref, rank ^ distance, count)
            block, low = blocks[head * count + distance], 0
            for ref, part in ((qg_ref, wide), (kg_ref, lanes), (vg_ref, lanes)):
                size = part.stop - part.start
                ref[index, :, part] = block[:, low : low + size]
                low += size
            for part in range(2):
                summed[part] = summed[part] + block[:, low : low + HEAD_DIM].astype(F32)
                low += HEAD_DIM
        pkg_ref[:, lanes] = summed[0][:prompt_rows].astype(BF16)
        pvg_ref[:, lanes] = summed[1][:prompt_rows].astype(BF16)


def exchange(blocks, distances, count):
    arrived = []
    for block, distance in zip(blocks, distances):
        if distance:
            block = lax.ppermute(block, "seq", [(i, i ^ distance) for i in range(count)])
        arrived.append(block)
    return arrived


def exchange_by_rank(blocks):
    return lax.all_to_all(blocks, "seq", split_axis=0, concat_axis=0, tiled=True)


SMEM = pl.BlockSpec(memory_space=pltpu.SMEM)
VMEM = pl.BlockSpec(memory_space=pltpu.VMEM)
HBM = pl.BlockSpec(memory_space=pltpu.HBM)
PARAMS = pltpu.CompilerParams(vmem_limit_bytes=24 * 1024 * 1024)


def packed_body(
    response_query,
    response_key,
    response_value,
    response_grad,
    prompt_key,
    prompt_value,
    lengths,
    home_rank,
    prompt_seen,
):
    count = home_rank.shape[0]
    rows, q_width = response_query.shape[1:]
    prompt_rows, kv_width = prompt_key.shape
    total = rows * count
    heads = kv_width // HEAD_DIM
    q_part = q_width // heads
    width = 2 * q_part + 4 * HEAD_DIM
    back = q_part + 4 * HEAD_DIM

    def shapes(by_rank, lanes):
        dims = [(count, rows, lanes)] if by_rank else [(rows, lanes)] * count
        return [jax.ShapeDtypeStruct(each, BF16) for each in dims]

    arrived = []
    sources = [
        pltpu.with_memory_space_constraint(source, pltpu.HBM)
        for source in (home_rank, response_query, response_key, response_value, response_grad, prompt_key, prompt_value)
    ]
    for head in range(heads):
        by_rank = head > 0
        results = shapes(by_rank, width)
        blocks = pl.pallas_call(
            functools.partial(pack_kernel, count=count, head=head, heads=heads, by_rank=by_rank),
            out_shape=results,
            in_specs=[HBM] * 7,
            out_specs=[VMEM] * len(results),
            scratch_shapes=[pltpu.SMEM((count,), jnp.int32)]
            + [pltpu.VMEM((count, rows, lanes), BF16) for lanes in (q_part, q_part, HEAD_DIM, HEAD_DIM)]
            + [pltpu.VMEM((2, prompt_rows, HEAD_DIM), BF16), pltpu.SemaphoreType.DMA((7,))],
            compiler_params=PARAMS,
        )(*sources)
        if by_rank:
            arrived.append([exchange_by_rank(blocks[0])])
        else:
            arrived.append(exchange(blocks, range(count), count))
    kept, returned = [], []
    for head in range(heads):
        last = head == heads - 1
        operands = [lengths, home_rank, prompt_seen, *arrived[head], *(kept if last else [])]
        whole = heads if last else 1
        results = [(1, total, whole * q_part)] + [(rows, back)] * count
        scratch = [back] if head else [width, back]
        results = pl.pallas_call(
            functools.partial(
                attend_kernel, count=count, prompt_rows=prompt_rows, head=head, heads=heads
            ),
            out_shape=[jax.ShapeDtypeStruct(dims, BF16) for dims in results],
            in_specs=[SMEM] * 3 + [VMEM] * (len(operands) - 3),
            out_specs=[VMEM] * len(results),
            scratch_shapes=[pltpu.VMEM((count, rows, lanes), BF16) for lanes in scratch],
            compiler_params=PARAMS,
        )(*operands)
        kept.append(results[0])
        returned += exchange(results[1:], range(count), count)
    output = kept[-1]
    grads = pl.pallas_call(
        functools.partial(unpack_kernel, count=count, heads=heads),
        name="unpack",
        out_shape=[
            jax.ShapeDtypeStruct(dims, BF16)
            for dims in ((count, rows, q_width), *[(count, rows, kv_width)] * 2, *[(prompt_rows, kv_width)] * 2)
        ],
        in_specs=[SMEM] + [VMEM] * len(returned),
        out_specs=[VMEM] * 5,
        compiler_params=PARAMS,
    )(home_rank, *returned)
    return (output, *grads)


def head_logits(queries, all_keys, allowed, head_index, group_size, scale_factor):
    row_count = queries.shape[0]
    low = head_index * group_size * HEAD_DIM
    high = (head_index + 1) * group_size * HEAD_DIM
    query_head = queries[:, low:high].reshape(row_count, group_size, HEAD_DIM)
    key_head = all_keys[:, head_index * HEAD_DIM : (head_index + 1) * HEAD_DIM]
    logits = (
        jnp.einsum("rhd,kd->rhk", query_head, key_head, preferred_element_type=jnp.float32)
        * scale_factor
    )
    return (query_head, key_head, jnp.where(allowed[:, None, :], logits, NEG_FILL))


def forward(queries, all_keys, all_values, allowed, live_rows, scale_factor):
    row_count = queries.shape[0]
    kv_count = all_keys.shape[1] // HEAD_DIM
    group_size = queries.shape[1] // all_keys.shape[1]
    outputs = []
    totals = []
    for head_index in range(kv_count):
        _, _, logits = head_logits(
            queries, all_keys, allowed, head_index, group_size, scale_factor
        )
        value_head = all_values[:, head_index * HEAD_DIM : (head_index + 1) * HEAD_DIM]
        row_max = jnp.max(logits, axis=2, keepdims=True)
        log_total = row_max + jnp.log(jnp.sum(jnp.exp(logits - row_max), axis=2, keepdims=True))
        weights = jnp.exp(logits - log_total).astype(jnp.bfloat16)
        mixed = jnp.einsum("rhk,kd->rhd", weights, value_head, preferred_element_type=jnp.float32)
        output_head = jnp.where(live_rows[:, None, None], mixed, 0.0).astype(jnp.bfloat16)
        outputs.append(output_head.reshape(row_count, group_size * HEAD_DIM))
        totals.append(log_total)
    return (jnp.concatenate(outputs, axis=1), totals)


def head_terms(grad_rows, live_rows, output, head_index, group_size):
    row_count = grad_rows.shape[0]
    low = head_index * group_size * HEAD_DIM
    high = (head_index + 1) * group_size * HEAD_DIM
    grad_head = jnp.where(live_rows[:, None], grad_rows[:, low:high], jnp.zeros((), jnp.bfloat16))
    grad_head = grad_head.reshape(row_count, group_size, HEAD_DIM)
    output_head = lax.optimization_barrier(output[:, low:high]).reshape(
        row_count, group_size, HEAD_DIM
    )
    row_dot = jnp.sum(
        grad_head.astype(jnp.float32) * output_head.astype(jnp.float32), axis=2, keepdims=True
    )
    return (grad_head, row_dot)


def backward(
    queries, all_keys, all_values, grad_rows, allowed, live_rows, output, totals, scale_factor
):
    row_count = queries.shape[0]
    kv_count = all_keys.shape[1] // HEAD_DIM
    group_size = queries.shape[1] // all_keys.shape[1]
    query_grads = []
    key_grads = []
    value_grads = []
    for head_index in range(kv_count):
        query_head, key_head, logits = head_logits(
            queries, all_keys, allowed, head_index, group_size, scale_factor
        )
        value_head = all_values[:, head_index * HEAD_DIM : (head_index + 1) * HEAD_DIM]
        prob = jnp.exp(logits - totals[head_index])
        weights = prob.astype(jnp.bfloat16)
        grad_head, row_dot = head_terms(grad_rows, live_rows, output, head_index, group_size)
        spread = jnp.einsum(
            "rhd,kd->rhk", grad_head, value_head, preferred_element_type=jnp.float32
        )
        dlogit = (prob * (spread - row_dot)).astype(jnp.bfloat16)
        query_part = (
            jnp.einsum("rhk,kd->rhd", dlogit, key_head, preferred_element_type=jnp.float32)
            * scale_factor
        )
        query_grads.append(query_part.reshape(row_count, group_size * HEAD_DIM))
        key_grads.append(
            jnp.einsum("rhk,rhd->kd", dlogit, query_head, preferred_element_type=jnp.float32)
            * scale_factor
        )
        value_grads.append(
            jnp.einsum("rhk,rhd->kd", weights, grad_head, preferred_element_type=jnp.float32)
        )
    return (
        jnp.concatenate(query_grads, axis=1),
        jnp.concatenate(key_grads, axis=1),
        jnp.concatenate(value_grads, axis=1),
    )


def body(
    response_query,
    response_key,
    response_value,
    response_grad,
    prompt_key,
    prompt_value,
    lengths,
    home_rank,
    prompt_seen,
):
    rank_count = home_rank.shape[0]
    rank_ids = jnp.arange(rank_count, dtype=jnp.int32)
    resident = jnp.sum(
        jnp.where(home_rank[None, :] == rank_ids[:, None], rank_ids[None, :], 0), axis=1
    )
    own_rank = lax.axis_index("seq")
    scale_factor = 1.0 / HEAD_DIM**0.5
    arrived = (
        lax.all_to_all(response_query[resident], "seq", split_axis=0, concat_axis=1, tiled=True),
        lax.all_to_all(response_key[resident], "seq", split_axis=0, concat_axis=1, tiled=True),
        lax.all_to_all(response_value[resident], "seq", split_axis=0, concat_axis=1, tiled=True),
        lax.all_to_all(response_grad[resident], "seq", split_axis=0, concat_axis=1, tiled=True),
    )
    queries = arrived[0][0]
    own_keys = arrived[1][0]
    own_values = arrived[2][0]
    grad_rows = arrived[3][0]
    own_response = resident[own_rank]
    length = lengths[own_response]
    visible = prompt_seen[own_response]
    max_length = queries.shape[0]
    prompt_rows = prompt_key.shape[0]
    prompt_total = prompt_rows * lax.axis_size("seq")
    positions = jnp.arange(max_length, dtype=jnp.int32)
    prompt_cols = jnp.arange(prompt_total, dtype=jnp.int32)
    seen_part = jnp.broadcast_to(prompt_cols[None, :] < visible, (max_length, prompt_total))
    allowed = jnp.concatenate([seen_part, positions[None, :] <= positions[:, None]], axis=1)
    live_rows = positions < length
    gathered_keys, gathered_values = (
        lax.all_gather(prompt_key, "seq", axis=0, tiled=True),
        lax.all_gather(prompt_value, "seq", axis=0, tiled=True),
    )
    all_keys = jnp.concatenate([gathered_keys, own_keys], axis=0)
    all_values = jnp.concatenate([gathered_values, own_values], axis=0)
    response_out, response_totals = forward(
        queries, all_keys, all_values, allowed, live_rows, scale_factor
    )
    query_grad, key_grad, value_grad = backward(
        queries,
        all_keys,
        all_values,
        grad_rows,
        allowed,
        live_rows,
        response_out,
        response_totals,
        scale_factor,
    )
    key_summed, value_summed = (
        lax.psum_scatter(key_grad[:prompt_total], "seq", scatter_dimension=0, tiled=True),
        lax.psum_scatter(value_grad[:prompt_total], "seq", scatter_dimension=0, tiled=True),
    )
    returned = (
        lax.all_to_all(
            query_grad.astype(jnp.bfloat16)[None], "seq", split_axis=1, concat_axis=0, tiled=True
        ),
        lax.all_to_all(
            key_grad[prompt_total:].astype(jnp.bfloat16)[None],
            "seq",
            split_axis=1,
            concat_axis=0,
            tiled=True,
        ),
        lax.all_to_all(
            value_grad[prompt_total:].astype(jnp.bfloat16)[None],
            "seq",
            split_axis=1,
            concat_axis=0,
            tiled=True,
        ),
    )
    return (
        response_out[None],
        returned[0][home_rank],
        returned[1][home_rank],
        returned[2][home_rank],
        key_summed.astype(jnp.bfloat16),
        value_summed.astype(jnp.bfloat16),
    )


def choose_body(response_query, *others):
    count, rows = response_query.shape[:2]
    prompt_rows = others[3].shape[0]
    fits = rows % 16 == 0 and prompt_rows <= rows and rows * count == HEAD_DIM
    if fits and count & (count - 1) == 0 and count <= 16:
        return packed_body(response_query, *others)
    return body(response_query, *others)


def solution(mesh):
    placed = (
        P("group", "seq", "head"),
        P("group", "seq", "head"),
        P("group", "seq", "head"),
        P("group", "seq", "head"),
        P(("group", "seq"), "head"),
        P(("group", "seq"), "head"),
        P("group"),
        P("group"),
        P("group"),
    )
    return jax.shard_map(
        choose_body,
        mesh=mesh,
        in_specs=placed,
        out_specs=(
            P(("group", "seq"), None, "head"),
            P("group", "seq", "head"),
            P("group", "seq", "head"),
            P("group", "seq", "head"),
            P(("group", "seq"), "head"),
            P(("group", "seq"), "head"),
        ),
        check_vma=False,
    )
```

```python
import functools

import jax
import jax.numpy as jnp
from jax import lax
from jax.experimental import pallas as pl
from jax.experimental.pallas import tpu as pltpu
from jax.sharding import PartitionSpec as P

HEAD_DIM = 128


NEG_FILL = -1e30
BF16 = jnp.bfloat16
F32 = jnp.float32


def resident_of(home_ref, rank, count):
    found = jnp.int32(0)
    for index in range(count):
        found = jnp.where(home_ref[index] == rank, jnp.int32(index), found)
    return found


def dot(left, right, contract):
    return lax.dot_general(left, right, ((contract[0], contract[1]), ((), ())), preferred_element_type=F32)


def padded_rows(ref, part, rows):
    spare = jnp.zeros((rows - ref.shape[1], ref.shape[2]), BF16)
    return jnp.concatenate([ref[part], spare], axis=0)


def pack_kernel(home_ref, q_ref, k_ref, v_ref, g_ref, pk_ref, pv_ref, *rest, count):
    blocks, (home, q, g, k, v, prompt, sems) = rest[:-7], rest[-7:]
    rank = lax.axis_index("seq")
    half = count // 2
    rows = q.shape[1]
    copies = [
        pltpu.make_async_copy(source, target, sems.at[index])
        for index, (source, target) in enumerate(
            (
                (home_ref, home),
                (q_ref, q),
                (g_ref, g),
                (k_ref, k),
                (v_ref, v),
                (pk_ref, prompt.at[0]),
                (pv_ref, prompt.at[1]),
            )
        )
    ]
    for copy in copies:
        copy.start()
    for copy in copies:
        copy.wait()
    padded = [padded_rows(prompt, part, rows) for part in range(2)]
    for distance in range(half):
        place = (rank ^ distance) & (half - 1)
        for part in range(2):
            index = resident_of(home, place + part * half, count)
            at = slice(part * rows, (part + 1) * rows)
            for block, refs in ((blocks[distance], (q, g, k, v)), (blocks[distance + half], (k, v))):
                low = 0
                for ref in refs:
                    block[at, low : low + ref.shape[2]] = ref[index]
                    low += ref.shape[2]
                block[at, low:] = padded[part]


def attend_kernel(lengths_ref, home_ref, seen_ref, *rest, count, prompt_rows, q_width, kv_width):
    half = count // 2
    blocks, rest = rest[:count], rest[count:]
    kept_ref, returns, (xq, xk, xp, o, yq, yk, yp) = rest[0], rest[1 : count + 1], rest[count + 1 :]
    rank = lax.axis_index("seq")
    place = rank & (half - 1)
    upper = rank // half
    rows = xk.shape[2]
    total = rows * count
    own_rows = rows * half
    heads = kv_width // HEAD_DIM
    members = q_width // kv_width
    scale = 1.0 / HEAD_DIM**0.5
    for distance in range(count):
        source = rank ^ distance
        for part in range(2):
            at = slice(part * rows, (part + 1) * rows)
            low = 0
            if distance < half:
                low = 2 * q_width
                xq[part, source & (half - 1)] = blocks[distance][at, :low]
            xk[part, source] = blocks[distance][at, low : low + 2 * kv_width]
            xp[part, source] = blocks[distance][at, low + 2 * kv_width :]
    column = lax.broadcasted_iota(jnp.int32, (own_rows, total), 1)
    position = lax.broadcasted_iota(jnp.int32, (own_rows, total), 0) + upper * own_rows
    shard_row = column % rows
    prompt_index = jnp.where(shard_row < prompt_rows, column // rows * prompt_rows + shard_row, 1 << 30)
    causal = column <= position
    allowed, live = [], []
    for part in range(2):
        index = resident_of(home_ref, place + part * half, count)
        mask = jnp.concatenate([prompt_index < seen_ref[index], causal], axis=1)
        allowed.append(jnp.concatenate([mask] * members, axis=0))
        rows_live = position[:, :HEAD_DIM] < lengths_ref[index]
        live.append(jnp.concatenate([rows_live] * members, axis=0))
    for kv in range(heads):
        lanes = slice(kv * HEAD_DIM, (kv + 1) * HEAD_DIM)
        wide = slice(kv_width + kv * HEAD_DIM, kv_width + (kv + 1) * HEAD_DIM)
        prompt_grads = [jnp.zeros((total, HEAD_DIM), F32)] * 2
        for part in range(2):

            def stacked(offset):
                lows = [offset + (kv * members + member) * HEAD_DIM for member in range(members)]
                return jnp.concatenate(
                    [xq[part, :, :, low : low + HEAD_DIM].reshape(own_rows, HEAD_DIM) for low in lows], axis=0
                )

            keys = jnp.concatenate(
                [xp[0, :, :, lanes].reshape(total, HEAD_DIM), xk[part, :, :, lanes].reshape(total, HEAD_DIM)], axis=0
            )
            values = jnp.concatenate(
                [xp[1, :, :, lanes].reshape(total, HEAD_DIM), xk[part, :, :, wide].reshape(total, HEAD_DIM)], axis=0
            )
            query = stacked(0)
            grad = jnp.where(live[part], stacked(q_width), jnp.zeros((), BF16))
            logits = jnp.where(allowed[part], dot(query, keys, ((1,), (1,))) * scale, NEG_FILL)
            spread = dot(grad, values, ((1,), (1,)))
            raised = jnp.exp(logits - jnp.max(logits, axis=1, keepdims=True))
            prob = raised * (1.0 / jnp.sum(raised, axis=1, keepdims=True))
            weights = prob.astype(BF16)
            output = jnp.where(live[part], dot(weights, values, ((1,), (0,))), 0.0).astype(BF16)
            row_dot = jnp.sum(grad.astype(F32) * output.astype(F32), axis=1, keepdims=True)
            dlogit = (prob * (spread - row_dot)).astype(BF16)
            query_grad = (dot(dlogit, keys, ((1,), (0,))) * scale).astype(BF16)
            for member in range(members):
                low = (kv * members + member) * HEAD_DIM
                at = slice(member * own_rows, (member + 1) * own_rows)
                o[part, :, low : low + HEAD_DIM] = output[at]
                yq[part, :, :, low : low + HEAD_DIM] = query_grad[at].reshape(half, rows, HEAD_DIM)
            summed = (dot(dlogit, query, ((0,), (0,))) * scale, dot(weights, grad, ((0,), (0,))))
            for index, to in enumerate((lanes, wide)):
                yk[part, :, :, to] = summed[index][total:].astype(BF16).reshape(count, rows, HEAD_DIM)
                prompt_grads[index] = prompt_grads[index] + summed[index][:total]
        for index in range(2):
            yp[index, :, :, lanes] = prompt_grads[index].astype(BF16).reshape(count, rows, HEAD_DIM)
    kept_ref[...] = o[upper]
    returns[half][:, :q_width] = o[1 - upper]
    for distance in range(count):
        target = rank ^ distance
        for part in range(2):
            at = slice(part * rows, (part + 1) * rows)
            if distance < half:
                returns[distance][at, :q_width] = yq[part, target & (half - 1)]
            terms = jnp.concatenate([yk[part, target], yp[part, target]], axis=1)
            if distance == half:
                fold = terms.shape[1] // 2
                returns[distance][at, q_width:] = terms[:, :fold]
                at = slice((2 + part) * rows, (3 + part) * rows)
                returns[distance][at, q_width:] = terms[:, fold:]
            else:
                returns[distance][at, q_width if distance < half else 0 :] = terms


def unpack_kernel(home_ref, kept_ref, *rest, count, q_width):
    half = count // 2
    blocks, (out_ref, qg_ref, kg_ref, vg_ref, pkg_ref, pvg_ref) = rest[:count], rest[count:]
    rank = lax.axis_index("seq")
    upper = rank // half
    own_rows = kept_ref.shape[0]
    rows = qg_ref.shape[1]
    prompt_rows, kv_width = pkg_ref.shape
    out_ref[0, pl.ds(pl.multiple_of(upper * own_rows, own_rows), own_rows), :] = kept_ref[...]
    other = pl.multiple_of((1 - upper) * own_rows, own_rows)
    out_ref[0, pl.ds(other, own_rows), :] = blocks[half][:own_rows, :q_width]
    prompt_grads = [jnp.zeros((rows, kv_width), F32)] * 2
    for distance in range(half):
        place = (rank ^ distance) & (half - 1)
        for part in range(2):
            index = resident_of(home_ref, place + part * half, count)
            at = slice(part * rows, (part + 1) * rows)
            qg_ref[index] = blocks[distance][at, :q_width]
            far = blocks[distance + half]
            if distance:
                far = far[at, :]
            else:
                far = jnp.concatenate(
                    [far[at, q_width:], far[(2 + part) * rows : (3 + part) * rows, q_width:]], axis=1
                )
            terms = blocks[distance][at, q_width:].astype(F32) + far.astype(F32)
            kg_ref[index] = terms[:, :kv_width].astype(BF16)
            vg_ref[index] = terms[:, kv_width : 2 * kv_width].astype(BF16)
            prompt_grads[part] = prompt_grads[part] + terms[:, 2 * kv_width :]
    pkg_ref[...] = prompt_grads[0][:prompt_rows].astype(BF16)
    pvg_ref[...] = prompt_grads[1][:prompt_rows].astype(BF16)


def exchange(blocks):
    count = len(blocks)
    arrived = list(blocks)
    for distance in range(1, count):
        arrived[distance] = lax.ppermute(
            blocks[distance], "seq", [(i, i ^ distance) for i in range(count)]
        )
    return arrived


SMEM = pl.BlockSpec(memory_space=pltpu.SMEM)
VMEM = pl.BlockSpec(memory_space=pltpu.VMEM)
HBM = pl.BlockSpec(memory_space=pltpu.HBM)
PARAMS = pltpu.CompilerParams(vmem_limit_bytes=32 * 1024 * 1024)


def packed_body(
    response_query,
    response_key,
    response_value,
    response_grad,
    prompt_key,
    prompt_value,
    lengths,
    home_rank,
    prompt_seen,
):
    count = home_rank.shape[0]
    half = count // 2
    rows, q_width = response_query.shape[1:]
    prompt_rows, kv_width = prompt_key.shape
    own_rows = rows * half
    terms = 3 * kv_width

    def shape(*dims):
        return jax.ShapeDtypeStruct(dims, BF16)

    def scratch(*dims):
        return pltpu.VMEM(dims, BF16)

    sources = [
        pltpu.with_memory_space_constraint(source, pltpu.HBM)
        for source in (home_rank, response_query, response_key, response_value, response_grad, prompt_key, prompt_value)
    ]
    blocks = pl.pallas_call(
        functools.partial(pack_kernel, count=count),
        name="pack",
        out_shape=[shape(2 * rows, 2 * q_width + terms)] * half + [shape(2 * rows, terms)] * half,
        in_specs=[HBM] * 7,
        out_specs=[VMEM] * count,
        scratch_shapes=[pltpu.SMEM((count,), jnp.int32)]
        + [scratch(count, rows, lanes) for lanes in (q_width, q_width, kv_width, kv_width)]
        + [scratch(2, prompt_rows, kv_width), pltpu.SemaphoreType.DMA((7,))],
        compiler_params=PARAMS,
    )(*sources)
    arrived = exchange(blocks)
    far_shapes = [shape(own_rows, q_width + 2 * rows * terms // own_rows)] + [shape(2 * rows, terms)] * (half - 1)
    kept, *returns = pl.pallas_call(
        functools.partial(
            attend_kernel, count=count, prompt_rows=prompt_rows, q_width=q_width, kv_width=kv_width
        ),
        name="attend",
        out_shape=[shape(own_rows, q_width)] + [shape(2 * rows, q_width + terms)] * half + far_shapes,
        in_specs=[SMEM] * 3 + [VMEM] * count,
        out_specs=[VMEM] * (count + 1),
        scratch_shapes=[
            scratch(2, half, rows, 2 * q_width),
            scratch(2, count, rows, 2 * kv_width),
            scratch(2, count, rows, kv_width),
            scratch(2, own_rows, q_width),
            scratch(2, half, rows, q_width),
            scratch(2, count, rows, 2 * kv_width),
            scratch(2, count, rows, kv_width),
        ],
        compiler_params=PARAMS,
    )(lengths, home_rank, prompt_seen, *arrived)
    returned = exchange(returns)
    return tuple(
        pl.pallas_call(
            functools.partial(unpack_kernel, count=count, q_width=q_width),
            name="unpack",
            out_shape=[shape(1, rows * count, q_width), shape(count, rows, q_width)]
            + [shape(count, rows, kv_width)] * 2
            + [shape(prompt_rows, kv_width)] * 2,
            in_specs=[SMEM] + [VMEM] * (count + 1),
            out_specs=[VMEM] * 6,
            compiler_params=PARAMS,
        )(home_rank, kept, *returned)
    )


def head_logits(queries, all_keys, allowed, head_index, group_size, scale_factor):
    row_count = queries.shape[0]
    low = head_index * group_size * HEAD_DIM
    high = (head_index + 1) * group_size * HEAD_DIM
    query_head = queries[:, low:high].reshape(row_count, group_size, HEAD_DIM)
    key_head = all_keys[:, head_index * HEAD_DIM : (head_index + 1) * HEAD_DIM]
    logits = (
        jnp.einsum("rhd,kd->rhk", query_head, key_head, preferred_element_type=jnp.float32)
        * scale_factor
    )
    return (query_head, key_head, jnp.where(allowed[:, None, :], logits, NEG_FILL))


def forward(queries, all_keys, all_values, allowed, live_rows, scale_factor):
    row_count = queries.shape[0]
    kv_count = all_keys.shape[1] // HEAD_DIM
    group_size = queries.shape[1] // all_keys.shape[1]
    outputs = []
    totals = []
    for head_index in range(kv_count):
        _, _, logits = head_logits(
            queries, all_keys, allowed, head_index, group_size, scale_factor
        )
        value_head = all_values[:, head_index * HEAD_DIM : (head_index + 1) * HEAD_DIM]
        row_max = jnp.max(logits, axis=2, keepdims=True)
        log_total = row_max + jnp.log(jnp.sum(jnp.exp(logits - row_max), axis=2, keepdims=True))
        weights = jnp.exp(logits - log_total).astype(jnp.bfloat16)
        mixed = jnp.einsum("rhk,kd->rhd", weights, value_head, preferred_element_type=jnp.float32)
        output_head = jnp.where(live_rows[:, None, None], mixed, 0.0).astype(jnp.bfloat16)
        outputs.append(output_head.reshape(row_count, group_size * HEAD_DIM))
        totals.append(log_total)
    return (jnp.concatenate(outputs, axis=1), totals)


def head_terms(grad_rows, live_rows, output, head_index, group_size):
    row_count = grad_rows.shape[0]
    low = head_index * group_size * HEAD_DIM
    high = (head_index + 1) * group_size * HEAD_DIM
    grad_head = jnp.where(live_rows[:, None], grad_rows[:, low:high], jnp.zeros((), jnp.bfloat16))
    grad_head = grad_head.reshape(row_count, group_size, HEAD_DIM)
    output_head = lax.optimization_barrier(output[:, low:high]).reshape(
        row_count, group_size, HEAD_DIM
    )
    row_dot = jnp.sum(
        grad_head.astype(jnp.float32) * output_head.astype(jnp.float32), axis=2, keepdims=True
    )
    return (grad_head, row_dot)


def backward(
    queries, all_keys, all_values, grad_rows, allowed, live_rows, output, totals, scale_factor
):
    row_count = queries.shape[0]
    kv_count = all_keys.shape[1] // HEAD_DIM
    group_size = queries.shape[1] // all_keys.shape[1]
    query_grads = []
    key_grads = []
    value_grads = []
    for head_index in range(kv_count):
        query_head, key_head, logits = head_logits(
            queries, all_keys, allowed, head_index, group_size, scale_factor
        )
        value_head = all_values[:, head_index * HEAD_DIM : (head_index + 1) * HEAD_DIM]
        prob = jnp.exp(logits - totals[head_index])
        weights = prob.astype(jnp.bfloat16)
        grad_head, row_dot = head_terms(grad_rows, live_rows, output, head_index, group_size)
        spread = jnp.einsum(
            "rhd,kd->rhk", grad_head, value_head, preferred_element_type=jnp.float32
        )
        dlogit = (prob * (spread - row_dot)).astype(jnp.bfloat16)
        query_part = (
            jnp.einsum("rhk,kd->rhd", dlogit, key_head, preferred_element_type=jnp.float32)
            * scale_factor
        )
        query_grads.append(query_part.reshape(row_count, group_size * HEAD_DIM))
        key_grads.append(
            jnp.einsum("rhk,rhd->kd", dlogit, query_head, preferred_element_type=jnp.float32)
            * scale_factor
        )
        value_grads.append(
            jnp.einsum("rhk,rhd->kd", weights, grad_head, preferred_element_type=jnp.float32)
        )
    return (
        jnp.concatenate(query_grads, axis=1),
        jnp.concatenate(key_grads, axis=1),
        jnp.concatenate(value_grads, axis=1),
    )


def body(
    response_query,
    response_key,
    response_value,
    response_grad,
    prompt_key,
    prompt_value,
    lengths,
    home_rank,
    prompt_seen,
):
    rank_count = home_rank.shape[0]
    rank_ids = jnp.arange(rank_count, dtype=jnp.int32)
    resident = jnp.sum(
        jnp.where(home_rank[None, :] == rank_ids[:, None], rank_ids[None, :], 0), axis=1
    )
    own_rank = lax.axis_index("seq")
    scale_factor = 1.0 / HEAD_DIM**0.5
    arrived = (
        lax.all_to_all(response_query[resident], "seq", split_axis=0, concat_axis=1, tiled=True),
        lax.all_to_all(response_key[resident], "seq", split_axis=0, concat_axis=1, tiled=True),
        lax.all_to_all(response_value[resident], "seq", split_axis=0, concat_axis=1, tiled=True),
        lax.all_to_all(response_grad[resident], "seq", split_axis=0, concat_axis=1, tiled=True),
    )
    queries = arrived[0][0]
    own_keys = arrived[1][0]
    own_values = arrived[2][0]
    grad_rows = arrived[3][0]
    own_response = resident[own_rank]
    length = lengths[own_response]
    visible = prompt_seen[own_response]
    max_length = queries.shape[0]
    prompt_rows = prompt_key.shape[0]
    prompt_total = prompt_rows * lax.axis_size("seq")
    positions = jnp.arange(max_length, dtype=jnp.int32)
    prompt_cols = jnp.arange(prompt_total, dtype=jnp.int32)
    seen_part = jnp.broadcast_to(prompt_cols[None, :] < visible, (max_length, prompt_total))
    allowed = jnp.concatenate([seen_part, positions[None, :] <= positions[:, None]], axis=1)
    live_rows = positions < length
    gathered_keys, gathered_values = (
        lax.all_gather(prompt_key, "seq", axis=0, tiled=True),
        lax.all_gather(prompt_value, "seq", axis=0, tiled=True),
    )
    all_keys = jnp.concatenate([gathered_keys, own_keys], axis=0)
    all_values = jnp.concatenate([gathered_values, own_values], axis=0)
    response_out, response_totals = forward(
        queries, all_keys, all_values, allowed, live_rows, scale_factor
    )
    query_grad, key_grad, value_grad = backward(
        queries,
        all_keys,
        all_values,
        grad_rows,
        allowed,
        live_rows,
        response_out,
        response_totals,
        scale_factor,
    )
    key_summed, value_summed = (
        lax.psum_scatter(key_grad[:prompt_total], "seq", scatter_dimension=0, tiled=True),
        lax.psum_scatter(value_grad[:prompt_total], "seq", scatter_dimension=0, tiled=True),
    )
    returned = (
        lax.all_to_all(
            query_grad.astype(jnp.bfloat16)[None], "seq", split_axis=1, concat_axis=0, tiled=True
        ),
        lax.all_to_all(
            key_grad[prompt_total:].astype(jnp.bfloat16)[None],
            "seq",
            split_axis=1,
            concat_axis=0,
            tiled=True,
        ),
        lax.all_to_all(
            value_grad[prompt_total:].astype(jnp.bfloat16)[None],
            "seq",
            split_axis=1,
            concat_axis=0,
            tiled=True,
        ),
    )
    return (
        response_out[None],
        returned[0][home_rank],
        returned[1][home_rank],
        returned[2][home_rank],
        key_summed.astype(jnp.bfloat16),
        value_summed.astype(jnp.bfloat16),
    )


def choose_body(response_query, *others):
    count, rows = response_query.shape[:2]
    prompt_rows = others[3].shape[0]
    fits = rows % 16 == 0 and prompt_rows <= rows and rows * count == HEAD_DIM
    if fits and count in (4, 8):
        return packed_body(response_query, *others)
    return body(response_query, *others)


def solution(mesh):
    placed = (
        P("group", "seq", "head"),
        P("group", "seq", "head"),
        P("group", "seq", "head"),
        P("group", "seq", "head"),
        P(("group", "seq"), "head"),
        P(("group", "seq"), "head"),
        P("group"),
        P("group"),
        P("group"),
    )
    return jax.shard_map(
        choose_body,
        mesh=mesh,
        in_specs=placed,
        out_specs=(
            P(("group", "seq"), None, "head"),
            P("group", "seq", "head"),
            P("group", "seq", "head"),
            P("group", "seq", "head"),
            P(("group", "seq"), "head"),
            P(("group", "seq"), "head"),
        ),
        check_vma=False,
    )
```

```python
import functools

import jax
import jax.numpy as jnp
from jax import lax
from jax.experimental import pallas as pl
from jax.experimental.pallas import tpu as pltpu
from jax.sharding import PartitionSpec as P

HEAD_DIM = 128


NEG_FILL = -1e30
BF16 = jnp.bfloat16
F32 = jnp.float32


def resident_of(home_ref, rank, count):
    found = jnp.int32(0)
    for index in range(count):
        found = jnp.where(home_ref[index] == rank, jnp.int32(index), found)
    return found


def dot(left, right, contract):
    return lax.dot_general(left, right, ((contract[0], contract[1]), ((), ())), preferred_element_type=F32)


def padded_rows(ref, part, rows):
    spare = jnp.zeros((rows - ref.shape[1], ref.shape[2]), BF16)
    return jnp.concatenate([ref[part], spare], axis=0)


def pack_kernel(home_ref, q_ref, k_ref, v_ref, g_ref, pk_ref, pv_ref, *rest, count, head, with_far):
    blocks, (home, q, g, k, v, prompt, sems) = rest[:-7], rest[-7:]
    rank = lax.axis_index("seq")
    half = count // 2
    rows, q_part = q.shape[1:]
    wide = pl.ds(head * q_part, q_part)
    copies = [
        pltpu.make_async_copy(source, target, sems.at[index])
        for index, (source, target) in enumerate(
            (
                (home_ref, home),
                (q_ref.at[:, :, wide], q),
                (g_ref.at[:, :, wide], g),
                (k_ref, k),
                (v_ref, v),
                (pk_ref, prompt.at[0]),
                (pv_ref, prompt.at[1]),
            )
        )
    ]
    for copy in copies:
        copy.start()
    for copy in copies:
        copy.wait()
    padded = [padded_rows(prompt, part, rows) for part in range(2)]
    lanes = slice(head * HEAD_DIM, (head + 1) * HEAD_DIM)
    for distance in range(half):
        place = (rank ^ distance) & (half - 1)
        for part in range(2):
            index = resident_of(home, place + part * half, count)
            at = slice(part * rows, (part + 1) * rows)
            near = [q[index], g[index], k[index, :, lanes], v[index, :, lanes], padded[part][:, lanes]]
            blocks[distance][at, :] = jnp.concatenate(near, axis=1)
            if with_far:
                blocks[distance + half][at, :] = jnp.concatenate([k[index], v[index], padded[part]], axis=1)


def attend_kernel(lengths_ref, home_ref, seen_ref, *rest, count, prompt_rows, head, heads):
    half = count // 2
    last = head == heads - 1
    blocks, rest = rest[:count], rest[count:]
    earlier, rest = (rest[: head * count], rest[head * count :]) if last else ((), rest)
    kept_ref, swap_ref, returns, rest = rest[0], rest[1], list(rest[2:-6]), rest[-6:]
    xq, xk, xp, yq, yk, yp = rest
    rank = lax.axis_index("seq")
    place = rank & (half - 1)
    upper = rank // half
    rows = xk.shape[2]
    total = rows * count
    own_rows = rows * half
    q_part = yq.shape[3]
    members = q_part // HEAD_DIM
    scale = 1.0 / HEAD_DIM**0.5
    for distance in range(count):
        source = rank ^ distance
        block = blocks[distance]
        for part in range(2):
            at = slice(part * rows, (part + 1) * rows)
            if distance < half:
                low, step = 2 * q_part, HEAD_DIM
                xq[part, source & (half - 1)] = block[at, :low]
            else:
                low, step = head * HEAD_DIM, heads * HEAD_DIM
            xk[part, source, :, :HEAD_DIM] = block[at, low : low + HEAD_DIM]
            xk[part, source, :, HEAD_DIM:] = block[at, low + step : low + step + HEAD_DIM]
            xp[part, source] = block[at, low + 2 * step : low + 2 * step + HEAD_DIM]
    column = lax.broadcasted_iota(jnp.int32, (own_rows, total), 1)
    position = lax.broadcasted_iota(jnp.int32, (own_rows, total), 0) + upper * own_rows
    shard_row = column % rows
    prompt_index = jnp.where(shard_row < prompt_rows, column // rows * prompt_rows + shard_row, 1 << 30)
    causal = column <= position
    prompt_grads = [jnp.zeros((total, HEAD_DIM), F32)] * 2
    outputs = []
    for part in range(2):
        index = resident_of(home_ref, place + part * half, count)
        mask = jnp.concatenate([prompt_index < seen_ref[index], causal], axis=1)
        allowed = jnp.concatenate([mask] * members, axis=0)
        live = jnp.concatenate([position[:, :HEAD_DIM] < lengths_ref[index]] * members, axis=0)

        def stacked(offset):
            return jnp.concatenate(
                [
                    xq[part, :, :, low : low + HEAD_DIM].reshape(own_rows, HEAD_DIM)
                    for low in range(offset, offset + q_part, HEAD_DIM)
                ],
                axis=0,
            )

        keys, values = (
            jnp.concatenate(
                [
                    xp[index].reshape(total, HEAD_DIM),
                    xk[part, :, :, index * HEAD_DIM : (index + 1) * HEAD_DIM].reshape(total, HEAD_DIM),
                ],
                axis=0,
            )
            for index in range(2)
        )
        query = stacked(0)
        grad = jnp.where(live, stacked(q_part), jnp.zeros((), BF16))
        logits = jnp.where(allowed, dot(query, keys, ((1,), (1,))) * scale, NEG_FILL)
        spread = dot(grad, values, ((1,), (1,)))
        raised = jnp.exp(logits - jnp.max(logits, axis=1, keepdims=True))
        prob = raised * (1.0 / jnp.sum(raised, axis=1, keepdims=True))
        weights = prob.astype(BF16)
        output = jnp.where(live, dot(weights, values, ((1,), (0,))), 0.0).astype(BF16)
        row_dot = jnp.sum(grad.astype(F32) * output.astype(F32), axis=1, keepdims=True)
        dlogit = (prob * (spread - row_dot)).astype(BF16)
        query_grad = (dot(dlogit, keys, ((1,), (0,))) * scale).astype(BF16)
        outputs.append(output)
        for member in range(members):
            at = slice(member * own_rows, (member + 1) * own_rows)
            yq[part, :, :, member * HEAD_DIM : (member + 1) * HEAD_DIM] = query_grad[at].reshape(half, rows, HEAD_DIM)
        summed = (dot(dlogit, query, ((0,), (0,))) * scale, dot(weights, grad, ((0,), (0,))))
        for index in range(2):
            to = slice(index * HEAD_DIM, (index + 1) * HEAD_DIM)
            yk[part, :, :, to] = summed[index][total:].astype(BF16).reshape(count, rows, HEAD_DIM)
            prompt_grads[index] = prompt_grads[index] + summed[index][:total]
    for index in range(2):
        yp[index] = prompt_grads[index].astype(BF16).reshape(count, rows, HEAD_DIM)
    stays = jnp.where(upper > 0, outputs[1], outputs[0])
    leaves = jnp.where(upper > 0, outputs[0], outputs[1])
    for member in range(members):
        at = slice(member * own_rows, (member + 1) * own_rows)
        lanes = slice(member * HEAD_DIM, (member + 1) * HEAD_DIM)
        kept_ref[:, lanes] = stays[at]
        swap_ref[:, lanes] = leaves[at]
    for distance in range(count):
        target = rank ^ distance
        near = distance < half
        for part in range(2):
            at = slice(part * rows, (part + 1) * rows)
            terms = [yk[part, target], yp[part, target]]
            if near:
                terms = [yq[part, target & (half - 1)], *terms]
            terms = [block[at, :] for block in earlier[distance::count]] + terms
            terms = jnp.concatenate(terms, axis=1)
            if last and distance == half:
                fold = terms.shape[1] // 2
                for index in range(2):
                    to = slice((2 * index + part) * rows, (2 * index + part + 1) * rows)
                    swap_ref[to, q_part:] = terms[:, index * fold : (index + 1) * fold]
            else:
                returns[distance - (last and distance > half)][at, :] = terms


def join_kernel(*rest, half, heads):
    kept, came, out_ref = rest[:heads], rest[heads:-1], rest[-1]
    own_rows, q_part = kept[0].shape
    upper = lax.axis_index("seq") // half
    own = pl.multiple_of(upper * own_rows, own_rows)
    other = pl.multiple_of((1 - upper) * own_rows, own_rows)
    for head in range(heads):
        lanes = slice(head * q_part, (head + 1) * q_part)
        out_ref[0, pl.ds(own, own_rows), lanes] = kept[head][...]
        out_ref[0, pl.ds(other, own_rows), lanes] = came[head][:, :q_part]


def unpack_kernel(home_ref, *rest, count, heads):
    half = count // 2
    blocks, (qg_ref, kg_ref, vg_ref, pkg_ref, pvg_ref) = rest[:count], rest[count:]
    rank = lax.axis_index("seq")
    rows, q_width = qg_ref.shape[1:]
    prompt_rows = pkg_ref.shape[0]
    q_part = q_width // heads
    near_size, far_size = q_part + 3 * HEAD_DIM, 3 * HEAD_DIM
    for head in range(heads):
        lanes = slice(head * HEAD_DIM, (head + 1) * HEAD_DIM)
        prompt_grads = [jnp.zeros((rows, HEAD_DIM), F32)] * 2
        for distance in range(half):
            place = (rank ^ distance) & (half - 1)
            for part in range(2):
                index = resident_of(home_ref, place + part * half, count)
                at = slice(part * rows, (part + 1) * rows)
                low = head * near_size
                qg_ref[index, :, head * q_part : (head + 1) * q_part] = blocks[distance][at, low : low + q_part]
                far = blocks[distance + half]
                if distance:
                    far = far[at, :]
                else:
                    far = jnp.concatenate(
                        [far[at, q_part:], far[(2 + part) * rows : (3 + part) * rows, q_part:]], axis=1
                    )
                far = far[:, head * far_size : (head + 1) * far_size]
                terms = blocks[distance][at, low + q_part : low + near_size].astype(F32) + far.astype(F32)
                kg_ref[index, :, lanes] = terms[:, :HEAD_DIM].astype(BF16)
                vg_ref[index, :, lanes] = terms[:, HEAD_DIM : 2 * HEAD_DIM].astype(BF16)
                prompt_grads[part] = prompt_grads[part] + terms[:, 2 * HEAD_DIM :]
        pkg_ref[:, lanes] = prompt_grads[0][:prompt_rows].astype(BF16)
        pvg_ref[:, lanes] = prompt_grads[1][:prompt_rows].astype(BF16)


def exchange(blocks, distances, count):
    arrived = []
    for block, distance in zip(blocks, distances, strict=True):
        if distance:
            block = lax.ppermute(block, "seq", [(i, i ^ distance) for i in range(count)])
        arrived.append(block)
    return arrived


SMEM = pl.BlockSpec(memory_space=pltpu.SMEM)
VMEM = pl.BlockSpec(memory_space=pltpu.VMEM)
HBM = pl.BlockSpec(memory_space=pltpu.HBM)
PARAMS = pltpu.CompilerParams(vmem_limit_bytes=32 * 1024 * 1024)


def packed_body(
    response_query,
    response_key,
    response_value,
    response_grad,
    prompt_key,
    prompt_value,
    lengths,
    home_rank,
    prompt_seen,
):
    count = home_rank.shape[0]
    half = count // 2
    rows, q_width = response_query.shape[1:]
    prompt_rows, kv_width = prompt_key.shape
    heads = kv_width // HEAD_DIM
    q_part = q_width // heads
    own_rows = rows * half
    near, far = range(half), range(half, count)
    far_size = 3 * HEAD_DIM
    near_size = q_part + far_size

    def shape(*dims):
        return jax.ShapeDtypeStruct(dims, BF16)

    def scratch(*dims):
        return pltpu.VMEM(dims, BF16)

    def call(kernel, results, operands, specs, spaces):
        made = pl.pallas_call(
            kernel,
            out_shape=results,
            in_specs=specs,
            out_specs=[VMEM] * len(results),
            scratch_shapes=spaces,
            compiler_params=PARAMS,
        )(*operands)
        return list(made)

    sources = [
        pltpu.with_memory_space_constraint(source, pltpu.HBM)
        for source in (home_rank, response_query, response_key, response_value, response_grad, prompt_key, prompt_value)
    ]
    near_in = []
    for head in range(heads):
        blocks = call(
            functools.partial(pack_kernel, count=count, head=head, with_far=head == 0),
            [shape(2 * rows, q_part + near_size)] * half + [shape(2 * rows, heads * far_size)] * (0 if head else half),
            sources,
            [HBM] * 7,
            [pltpu.SMEM((count,), jnp.int32)]
            + [scratch(count, rows, lanes) for lanes in (q_part, q_part, kv_width, kv_width)]
            + [scratch(2, prompt_rows, kv_width), pltpu.SemaphoreType.DMA((7,))],
        )
        near_in.append(exchange(blocks[:half], near, count))
        if head == 0:
            far_in = exchange(blocks[half:], far, count)
    kept, came, returns = [], [], []
    for head in range(heads):
        last = head == heads - 1
        operands = [lengths, home_rank, prompt_seen, *near_in[head], *far_in, *(returns if last else [])]
        whole = heads if last else 1
        fold = 2 * rows * whole * far_size // own_rows if last else 0
        results = call(
            functools.partial(attend_kernel, count=count, prompt_rows=prompt_rows, head=head, heads=heads),
            [shape(own_rows, q_part), shape(own_rows, q_part + fold)]
            + [shape(2 * rows, whole * near_size)] * half
            + [shape(2 * rows, whole * far_size)] * (half - last),
            operands,
            [SMEM] * 3 + [VMEM] * (len(operands) - 3),
            [
                scratch(2, half, rows, 2 * q_part),
                scratch(2, count, rows, 2 * HEAD_DIM),
                scratch(2, count, rows, HEAD_DIM),
                scratch(2, half, rows, q_part),
                scratch(2, count, rows, 2 * HEAD_DIM),
                scratch(2, count, rows, HEAD_DIM),
            ],
        )
        kept.append(results[0])
        came += exchange(results[1:2], [half], count)
        returns = returns + results[2:] if not last else results[2:]
    returned = exchange(returns, [*near, *far[1:]], count)
    returned.insert(half, came[-1])
    output = call(
        functools.partial(join_kernel, half=half, heads=heads),
        [shape(1, rows * count, q_width)],
        [*kept, *came],
        [VMEM] * (2 * heads),
        [],
    )
    grads = call(
        functools.partial(unpack_kernel, count=count, heads=heads),
        [shape(count, rows, q_width)] + [shape(count, rows, kv_width)] * 2 + [shape(prompt_rows, kv_width)] * 2,
        [home_rank, *returned],
        [SMEM] + [VMEM] * count,
        [],
    )
    return (*output, *grads)


def head_logits(queries, all_keys, allowed, head_index, group_size, scale_factor):
    row_count = queries.shape[0]
    low = head_index * group_size * HEAD_DIM
    high = (head_index + 1) * group_size * HEAD_DIM
    query_head = queries[:, low:high].reshape(row_count, group_size, HEAD_DIM)
    key_head = all_keys[:, head_index * HEAD_DIM : (head_index + 1) * HEAD_DIM]
    logits = (
        jnp.einsum("rhd,kd->rhk", query_head, key_head, preferred_element_type=jnp.float32)
        * scale_factor
    )
    return (query_head, key_head, jnp.where(allowed[:, None, :], logits, NEG_FILL))


def forward(queries, all_keys, all_values, allowed, live_rows, scale_factor):
    row_count = queries.shape[0]
    kv_count = all_keys.shape[1] // HEAD_DIM
    group_size = queries.shape[1] // all_keys.shape[1]
    outputs = []
    totals = []
    for head_index in range(kv_count):
        _, _, logits = head_logits(
            queries, all_keys, allowed, head_index, group_size, scale_factor
        )
        value_head = all_values[:, head_index * HEAD_DIM : (head_index + 1) * HEAD_DIM]
        row_max = jnp.max(logits, axis=2, keepdims=True)
        log_total = row_max + jnp.log(jnp.sum(jnp.exp(logits - row_max), axis=2, keepdims=True))
        weights = jnp.exp(logits - log_total).astype(jnp.bfloat16)
        mixed = jnp.einsum("rhk,kd->rhd", weights, value_head, preferred_element_type=jnp.float32)
        output_head = jnp.where(live_rows[:, None, None], mixed, 0.0).astype(jnp.bfloat16)
        outputs.append(output_head.reshape(row_count, group_size * HEAD_DIM))
        totals.append(log_total)
    return (jnp.concatenate(outputs, axis=1), totals)


def head_terms(grad_rows, live_rows, output, head_index, group_size):
    row_count = grad_rows.shape[0]
    low = head_index * group_size * HEAD_DIM
    high = (head_index + 1) * group_size * HEAD_DIM
    grad_head = jnp.where(live_rows[:, None], grad_rows[:, low:high], jnp.zeros((), jnp.bfloat16))
    grad_head = grad_head.reshape(row_count, group_size, HEAD_DIM)
    output_head = lax.optimization_barrier(output[:, low:high]).reshape(
        row_count, group_size, HEAD_DIM
    )
    row_dot = jnp.sum(
        grad_head.astype(jnp.float32) * output_head.astype(jnp.float32), axis=2, keepdims=True
    )
    return (grad_head, row_dot)


def backward(
    queries, all_keys, all_values, grad_rows, allowed, live_rows, output, totals, scale_factor
):
    row_count = queries.shape[0]
    kv_count = all_keys.shape[1] // HEAD_DIM
    group_size = queries.shape[1] // all_keys.shape[1]
    query_grads = []
    key_grads = []
    value_grads = []
    for head_index in range(kv_count):
        query_head, key_head, logits = head_logits(
            queries, all_keys, allowed, head_index, group_size, scale_factor
        )
        value_head = all_values[:, head_index * HEAD_DIM : (head_index + 1) * HEAD_DIM]
        prob = jnp.exp(logits - totals[head_index])
        weights = prob.astype(jnp.bfloat16)
        grad_head, row_dot = head_terms(grad_rows, live_rows, output, head_index, group_size)
        spread = jnp.einsum(
            "rhd,kd->rhk", grad_head, value_head, preferred_element_type=jnp.float32
        )
        dlogit = (prob * (spread - row_dot)).astype(jnp.bfloat16)
        query_part = (
            jnp.einsum("rhk,kd->rhd", dlogit, key_head, preferred_element_type=jnp.float32)
            * scale_factor
        )
        query_grads.append(query_part.reshape(row_count, group_size * HEAD_DIM))
        key_grads.append(
            jnp.einsum("rhk,rhd->kd", dlogit, query_head, preferred_element_type=jnp.float32)
            * scale_factor
        )
        value_grads.append(
            jnp.einsum("rhk,rhd->kd", weights, grad_head, preferred_element_type=jnp.float32)
        )
    return (
        jnp.concatenate(query_grads, axis=1),
        jnp.concatenate(key_grads, axis=1),
        jnp.concatenate(value_grads, axis=1),
    )


def body(
    response_query,
    response_key,
    response_value,
    response_grad,
    prompt_key,
    prompt_value,
    lengths,
    home_rank,
    prompt_seen,
):
    rank_count = home_rank.shape[0]
    rank_ids = jnp.arange(rank_count, dtype=jnp.int32)
    resident = jnp.sum(
        jnp.where(home_rank[None, :] == rank_ids[:, None], rank_ids[None, :], 0), axis=1
    )
    own_rank = lax.axis_index("seq")
    scale_factor = 1.0 / HEAD_DIM**0.5
    arrived = (
        lax.all_to_all(response_query[resident], "seq", split_axis=0, concat_axis=1, tiled=True),
        lax.all_to_all(response_key[resident], "seq", split_axis=0, concat_axis=1, tiled=True),
        lax.all_to_all(response_value[resident], "seq", split_axis=0, concat_axis=1, tiled=True),
        lax.all_to_all(response_grad[resident], "seq", split_axis=0, concat_axis=1, tiled=True),
    )
    queries = arrived[0][0]
    own_keys = arrived[1][0]
    own_values = arrived[2][0]
    grad_rows = arrived[3][0]
    own_response = resident[own_rank]
    length = lengths[own_response]
    visible = prompt_seen[own_response]
    max_length = queries.shape[0]
    prompt_rows = prompt_key.shape[0]
    prompt_total = prompt_rows * lax.axis_size("seq")
    positions = jnp.arange(max_length, dtype=jnp.int32)
    prompt_cols = jnp.arange(prompt_total, dtype=jnp.int32)
    seen_part = jnp.broadcast_to(prompt_cols[None, :] < visible, (max_length, prompt_total))
    allowed = jnp.concatenate([seen_part, positions[None, :] <= positions[:, None]], axis=1)
    live_rows = positions < length
    gathered_keys, gathered_values = (
        lax.all_gather(prompt_key, "seq", axis=0, tiled=True),
        lax.all_gather(prompt_value, "seq", axis=0, tiled=True),
    )
    all_keys = jnp.concatenate([gathered_keys, own_keys], axis=0)
    all_values = jnp.concatenate([gathered_values, own_values], axis=0)
    response_out, response_totals = forward(
        queries, all_keys, all_values, allowed, live_rows, scale_factor
    )
    query_grad, key_grad, value_grad = backward(
        queries,
        all_keys,
        all_values,
        grad_rows,
        allowed,
        live_rows,
        response_out,
        response_totals,
        scale_factor,
    )
    key_summed, value_summed = (
        lax.psum_scatter(key_grad[:prompt_total], "seq", scatter_dimension=0, tiled=True),
        lax.psum_scatter(value_grad[:prompt_total], "seq", scatter_dimension=0, tiled=True),
    )
    returned = (
        lax.all_to_all(
            query_grad.astype(jnp.bfloat16)[None], "seq", split_axis=1, concat_axis=0, tiled=True
        ),
        lax.all_to_all(
            key_grad[prompt_total:].astype(jnp.bfloat16)[None],
            "seq",
            split_axis=1,
            concat_axis=0,
            tiled=True,
        ),
        lax.all_to_all(
            value_grad[prompt_total:].astype(jnp.bfloat16)[None],
            "seq",
            split_axis=1,
            concat_axis=0,
            tiled=True,
        ),
    )
    return (
        response_out[None],
        returned[0][home_rank],
        returned[1][home_rank],
        returned[2][home_rank],
        key_summed.astype(jnp.bfloat16),
        value_summed.astype(jnp.bfloat16),
    )


def choose_body(response_query, *others):
    count, rows = response_query.shape[:2]
    prompt_rows = others[3].shape[0]
    fits = rows % 16 == 0 and prompt_rows <= rows and rows * count == HEAD_DIM
    if fits and count in (4, 8):
        return packed_body(response_query, *others)
    return body(response_query, *others)


def solution(mesh):
    placed = (
        P("group", "seq", "head"),
        P("group", "seq", "head"),
        P("group", "seq", "head"),
        P("group", "seq", "head"),
        P(("group", "seq"), "head"),
        P(("group", "seq"), "head"),
        P("group"),
        P("group"),
        P("group"),
    )
    return jax.shard_map(
        choose_body,
        mesh=mesh,
        in_specs=placed,
        out_specs=(
            P(("group", "seq"), None, "head"),
            P("group", "seq", "head"),
            P("group", "seq", "head"),
            P("group", "seq", "head"),
            P(("group", "seq"), "head"),
            P(("group", "seq"), "head"),
        ),
        check_vma=False,
    )
```

```python
import functools

import jax
import jax.numpy as jnp
from jax import lax
from jax.experimental import pallas as pl
from jax.experimental.pallas import tpu as pltpu
from jax.sharding import PartitionSpec as P

HEAD_DIM = 128


NEG_FILL = -1e30
BF16 = jnp.bfloat16
F32 = jnp.float32


def resident_of(home_ref, rank, count):
    found = jnp.int32(0)
    for index in range(count):
        found = jnp.where(home_ref[index] == rank, jnp.int32(index), found)
    return found


def dot(left, right, contract):
    return lax.dot_general(left, right, ((contract[0], contract[1]), ((), ())), preferred_element_type=F32)


def padded_rows(ref, part, rows):
    spare = jnp.zeros((rows - ref.shape[1], ref.shape[2]), BF16)
    return jnp.concatenate([ref[part], spare], axis=0)


def pack_kernel(home_ref, q_ref, k_ref, v_ref, g_ref, pk_ref, pv_ref, *rest, count, heads):
    blocks, (home, q, g, k, v, prompt, sems) = rest[:-7], rest[-7:]
    rank = lax.axis_index("seq")
    half = count // 2
    rows = q.shape[1]
    q_part = q.shape[2] // heads
    copies = [
        pltpu.make_async_copy(source, target, sems.at[index])
        for index, (source, target) in enumerate(
            (
                (home_ref, home),
                (q_ref, q),
                (g_ref, g),
                (k_ref, k),
                (v_ref, v),
                (pk_ref, prompt.at[0]),
                (pv_ref, prompt.at[1]),
            )
        )
    ]
    for copy in copies:
        copy.start()
    for copy in copies:
        copy.wait()
    padded = [padded_rows(prompt, part, rows) for part in range(2)]
    for distance in range(half):
        place = (rank ^ distance) & (half - 1)
        for part in range(2):
            index = resident_of(home, place + part * half, count)
            at = slice(part * rows, (part + 1) * rows)
            for head in range(heads):
                lanes = slice(head * HEAD_DIM, (head + 1) * HEAD_DIM)
                wide = slice(head * q_part, (head + 1) * q_part)
                near = [ref[index, :, of] for ref, of in ((q, wide), (g, wide), (k, lanes), (v, lanes))]
                blocks[head * half + distance][at, :] = jnp.concatenate([*near, padded[part][:, lanes]], axis=1)
            far = [k[index], v[index], padded[part]]
            blocks[heads * half + distance][at, :] = jnp.concatenate(far, axis=1)


def folded(part, tile, rows, half, q_part):
    row_block, lane_block = (3 * part + tile) % half, (3 * part + tile) // half
    low = q_part + lane_block * HEAD_DIM
    return slice(row_block * rows, (row_block + 1) * rows), slice(low, low + HEAD_DIM)


def attend_kernel(lengths_ref, home_ref, seen_ref, *rest, count, prompt_rows, head, heads):
    half = count // 2
    last = head == heads - 1
    blocks, rest = rest[:count], rest[count:]
    carried = head * (half - 1) if last else 0
    earlier, rest = rest[:carried], rest[carried:]
    kept_ref, swap_ref, returns, rest = rest[0], rest[1], list(rest[2:-6]), rest[-6:]
    xq, xk, xp, yq, yk, yp = rest
    rank = lax.axis_index("seq")
    place = rank & (half - 1)
    upper = rank // half
    rows = xk.shape[2]
    total = rows * count
    own_rows = rows * half
    q_part = yq.shape[3]
    members = q_part // HEAD_DIM
    scale = 1.0 / HEAD_DIM**0.5
    for distance in range(count):
        source = rank ^ distance
        block = blocks[distance]
        for part in range(2):
            at = slice(part * rows, (part + 1) * rows)
            if distance < half:
                low, step = 2 * q_part, HEAD_DIM
                xq[part, source & (half - 1)] = block[at, :low]
            else:
                low, step = head * HEAD_DIM, heads * HEAD_DIM
            xk[part, source, :, :HEAD_DIM] = block[at, low : low + HEAD_DIM]
            xk[part, source, :, HEAD_DIM:] = block[at, low + step : low + step + HEAD_DIM]
            xp[part, source] = block[at, low + 2 * step : low + 2 * step + HEAD_DIM]
    column = lax.broadcasted_iota(jnp.int32, (own_rows, total), 1)
    position = lax.broadcasted_iota(jnp.int32, (own_rows, total), 0) + upper * own_rows
    shard_row = column % rows
    prompt_index = jnp.where(shard_row < prompt_rows, column // rows * prompt_rows + shard_row, 1 << 30)
    causal = column <= position
    prompt_grads = [jnp.zeros((total, HEAD_DIM), F32)] * 2
    outputs = []
    for part in range(2):
        index = resident_of(home_ref, place + part * half, count)
        mask = jnp.concatenate([prompt_index < seen_ref[index], causal], axis=1)
        allowed = jnp.concatenate([mask] * members, axis=0)
        live = jnp.concatenate([position[:, :HEAD_DIM] < lengths_ref[index]] * members, axis=0)

        def stacked(offset):
            return jnp.concatenate(
                [
                    xq[part, :, :, low : low + HEAD_DIM].reshape(own_rows, HEAD_DIM)
                    for low in range(offset, offset + q_part, HEAD_DIM)
                ],
                axis=0,
            )

        keys, values = (
            jnp.concatenate(
                [
                    xp[index].reshape(total, HEAD_DIM),
                    xk[part, :, :, index * HEAD_DIM : (index + 1) * HEAD_DIM].reshape(total, HEAD_DIM),
                ],
                axis=0,
            )
            for index in range(2)
        )
        query = stacked(0)
        grad = jnp.where(live, stacked(q_part), jnp.zeros((), BF16))
        logits = jnp.where(allowed, dot(query, keys, ((1,), (1,))) * scale, NEG_FILL)
        spread = dot(grad, values, ((1,), (1,)))
        raised = jnp.exp(logits - jnp.max(logits, axis=1, keepdims=True))
        prob = raised * (1.0 / jnp.sum(raised, axis=1, keepdims=True))
        weights = prob.astype(BF16)
        output = jnp.where(live, dot(weights, values, ((1,), (0,))), 0.0).astype(BF16)
        row_dot = jnp.sum(grad.astype(F32) * output.astype(F32), axis=1, keepdims=True)
        dlogit = (prob * (spread - row_dot)).astype(BF16)
        query_grad = (dot(dlogit, keys, ((1,), (0,))) * scale).astype(BF16)
        outputs.append(output)
        for member in range(members):
            at = slice(member * own_rows, (member + 1) * own_rows)
            yq[part, :, :, member * HEAD_DIM : (member + 1) * HEAD_DIM] = query_grad[at].reshape(half, rows, HEAD_DIM)
        summed = (dot(dlogit, query, ((0,), (0,))) * scale, dot(weights, grad, ((0,), (0,))))
        for index in range(2):
            to = slice(index * HEAD_DIM, (index + 1) * HEAD_DIM)
            yk[part, :, :, to] = summed[index][total:].astype(BF16).reshape(count, rows, HEAD_DIM)
            prompt_grads[index] = prompt_grads[index] + summed[index][:total]
    for index in range(2):
        yp[index] = prompt_grads[index].astype(BF16).reshape(count, rows, HEAD_DIM)
    stays = jnp.where(upper > 0, outputs[1], outputs[0])
    leaves = jnp.where(upper > 0, outputs[0], outputs[1])
    for member in range(members):
        at = slice(member * own_rows, (member + 1) * own_rows)
        lanes = slice(member * HEAD_DIM, (member + 1) * HEAD_DIM)
        kept_ref[:, lanes] = stays[at]
        swap_ref[:, lanes] = leaves[at]
    for distance in range(count):
        target = rank ^ distance
        near = distance < half
        for part in range(2):
            at = slice(part * rows, (part + 1) * rows)
            terms = [yk[part, target], yp[part, target]]
            if near:
                terms = [yq[part, target & (half - 1)], *terms]
            elif distance > half:
                terms = [block[at, :] for block in earlier[distance - half - 1 :: half - 1]] + terms
            terms = jnp.concatenate(terms, axis=1)
            if distance == half:
                for tile in range(3):
                    to_rows, to_lanes = folded(part, tile, rows, half, q_part)
                    swap_ref[to_rows, to_lanes] = terms[:, tile * HEAD_DIM : (tile + 1) * HEAD_DIM]
            else:
                returns[distance - (distance > half)][at, :] = terms


def join_kernel(*rest, half, heads):
    kept, came, out_ref = rest[:heads], rest[heads:-1], rest[-1]
    own_rows, q_part = kept[0].shape
    upper = lax.axis_index("seq") // half
    own = pl.multiple_of(upper * own_rows, own_rows)
    other = pl.multiple_of((1 - upper) * own_rows, own_rows)
    for head in range(heads):
        lanes = slice(head * q_part, (head + 1) * q_part)
        out_ref[0, pl.ds(own, own_rows), lanes] = kept[head][...]
        out_ref[0, pl.ds(other, own_rows), lanes] = came[head][:, :q_part]


def unpack_kernel(home_ref, *rest, count, heads):
    half = count // 2
    blocks, (qg_ref, kg_ref, vg_ref, pkg_ref, pvg_ref) = rest[:-5], rest[-5:]
    near, came, far = blocks[: heads * half], blocks[heads * half : heads * (half + 1)], blocks[heads * (half + 1) :]
    rank = lax.axis_index("seq")
    rows, q_width = qg_ref.shape[1:]
    prompt_rows = pkg_ref.shape[0]
    q_part = q_width // heads
    far_size = 3 * HEAD_DIM
    for head in range(heads):
        lanes = slice(head * HEAD_DIM, (head + 1) * HEAD_DIM)
        prompt_grads = [jnp.zeros((rows, HEAD_DIM), F32)] * 2
        for distance in range(half):
            place = (rank ^ distance) & (half - 1)
            block = near[head * half + distance]
            for part in range(2):
                index = resident_of(home_ref, place + part * half, count)
                at = slice(part * rows, (part + 1) * rows)
                qg_ref[index, :, head * q_part : (head + 1) * q_part] = block[at, :q_part]
                if distance:
                    other = far[distance - 1][at, head * far_size : (head + 1) * far_size]
                else:
                    spots = [folded(part, tile, rows, half, q_part) for tile in range(3)]
                    other = jnp.concatenate([came[head][spot] for spot in spots], axis=1)
                terms = block[at, q_part:].astype(F32) + other.astype(F32)
                kg_ref[index, :, lanes] = terms[:, :HEAD_DIM].astype(BF16)
                vg_ref[index, :, lanes] = terms[:, HEAD_DIM : 2 * HEAD_DIM].astype(BF16)
                prompt_grads[part] = prompt_grads[part] + terms[:, 2 * HEAD_DIM :]
        pkg_ref[:, lanes] = prompt_grads[0][:prompt_rows].astype(BF16)
        pvg_ref[:, lanes] = prompt_grads[1][:prompt_rows].astype(BF16)


def exchange(blocks, distances, count):
    arrived = []
    for block, distance in zip(blocks, distances, strict=True):
        if distance:
            block = lax.ppermute(block, "seq", [(i, i ^ distance) for i in range(count)])
        arrived.append(block)
    return arrived


SMEM = pl.BlockSpec(memory_space=pltpu.SMEM)
VMEM = pl.BlockSpec(memory_space=pltpu.VMEM)
HBM = pl.BlockSpec(memory_space=pltpu.HBM)
PARAMS = pltpu.CompilerParams(vmem_limit_bytes=32 * 1024 * 1024)


def packed_body(
    response_query,
    response_key,
    response_value,
    response_grad,
    prompt_key,
    prompt_value,
    lengths,
    home_rank,
    prompt_seen,
):
    count = home_rank.shape[0]
    half = count // 2
    rows, q_width = response_query.shape[1:]
    prompt_rows, kv_width = prompt_key.shape
    heads = kv_width // HEAD_DIM
    q_part = q_width // heads
    own_rows = rows * half
    near, far = range(half), range(half, count)
    far_size = 3 * HEAD_DIM
    near_size = q_part + far_size

    def shape(*dims):
        return jax.ShapeDtypeStruct(dims, BF16)

    def scratch(*dims):
        return pltpu.VMEM(dims, BF16)

    def call(kernel, results, operands, specs, spaces):
        made = pl.pallas_call(
            kernel,
            out_shape=results,
            in_specs=specs,
            out_specs=[VMEM] * len(results),
            scratch_shapes=spaces,
            compiler_params=PARAMS,
        )(*operands)
        return list(made)

    sources = [
        pltpu.with_memory_space_constraint(source, pltpu.HBM)
        for source in (home_rank, response_query, response_key, response_value, response_grad, prompt_key, prompt_value)
    ]
    blocks = call(
        functools.partial(pack_kernel, count=count, heads=heads),
        [shape(2 * rows, q_part + near_size)] * (heads * half) + [shape(2 * rows, heads * far_size)] * half,
        sources,
        [HBM] * 7,
        [pltpu.SMEM((count,), jnp.int32)]
        + [scratch(count, rows, lanes) for lanes in (q_width, q_width, kv_width, kv_width)]
        + [scratch(2, prompt_rows, kv_width), pltpu.SemaphoreType.DMA((7,))],
    )
    near_in = [exchange(blocks[head * half : (head + 1) * half], near, count) for head in range(heads)]
    far_in = exchange(blocks[heads * half :], far, count)
    kept, came, near_back, far_back = [], [], [], []
    beside = -(-6 // half) * HEAD_DIM
    for head in range(heads):
        last = head == heads - 1
        operands = [lengths, home_rank, prompt_seen, *near_in[head], *far_in, *(far_back if last else [])]
        whole = heads if last else 1
        results = call(
            functools.partial(attend_kernel, count=count, prompt_rows=prompt_rows, head=head, heads=heads),
            [shape(own_rows, q_part), shape(own_rows, q_part + beside)]
            + [shape(2 * rows, near_size)] * half
            + [shape(2 * rows, whole * far_size)] * (half - 1),
            operands,
            [SMEM] * 3 + [VMEM] * (len(operands) - 3),
            [
                scratch(2, half, rows, 2 * q_part),
                scratch(2, count, rows, 2 * HEAD_DIM),
                scratch(2, count, rows, HEAD_DIM),
                scratch(2, half, rows, q_part),
                scratch(2, count, rows, 2 * HEAD_DIM),
                scratch(2, count, rows, HEAD_DIM),
            ],
        )
        kept.append(results[0])
        came += exchange(results[1:2], [half], count)
        near_back += exchange(results[2 : 2 + half], near, count)
        far_back = [*([] if last else far_back), *results[2 + half :]]
    returned = [*near_back, *came, *exchange(far_back, far[1:], count)]
    output = call(
        functools.partial(join_kernel, half=half, heads=heads),
        [shape(1, rows * count, q_width)],
        [*kept, *came],
        [VMEM] * (2 * heads),
        [],
    )
    grads = call(
        functools.partial(unpack_kernel, count=count, heads=heads),
        [shape(count, rows, q_width)] + [shape(count, rows, kv_width)] * 2 + [shape(prompt_rows, kv_width)] * 2,
        [home_rank, *returned],
        [SMEM] + [VMEM] * len(returned),
        [],
    )
    return (*output, *grads)


def head_logits(queries, all_keys, allowed, head_index, group_size, scale_factor):
    row_count = queries.shape[0]
    low = head_index * group_size * HEAD_DIM
    high = (head_index + 1) * group_size * HEAD_DIM
    query_head = queries[:, low:high].reshape(row_count, group_size, HEAD_DIM)
    key_head = all_keys[:, head_index * HEAD_DIM : (head_index + 1) * HEAD_DIM]
    logits = (
        jnp.einsum("rhd,kd->rhk", query_head, key_head, preferred_element_type=jnp.float32)
        * scale_factor
    )
    return (query_head, key_head, jnp.where(allowed[:, None, :], logits, NEG_FILL))


def forward(queries, all_keys, all_values, allowed, live_rows, scale_factor):
    row_count = queries.shape[0]
    kv_count = all_keys.shape[1] // HEAD_DIM
    group_size = queries.shape[1] // all_keys.shape[1]
    outputs = []
    totals = []
    for head_index in range(kv_count):
        _, _, logits = head_logits(
            queries, all_keys, allowed, head_index, group_size, scale_factor
        )
        value_head = all_values[:, head_index * HEAD_DIM : (head_index + 1) * HEAD_DIM]
        row_max = jnp.max(logits, axis=2, keepdims=True)
        log_total = row_max + jnp.log(jnp.sum(jnp.exp(logits - row_max), axis=2, keepdims=True))
        weights = jnp.exp(logits - log_total).astype(jnp.bfloat16)
        mixed = jnp.einsum("rhk,kd->rhd", weights, value_head, preferred_element_type=jnp.float32)
        output_head = jnp.where(live_rows[:, None, None], mixed, 0.0).astype(jnp.bfloat16)
        outputs.append(output_head.reshape(row_count, group_size * HEAD_DIM))
        totals.append(log_total)
    return (jnp.concatenate(outputs, axis=1), totals)


def head_terms(grad_rows, live_rows, output, head_index, group_size):
    row_count = grad_rows.shape[0]
    low = head_index * group_size * HEAD_DIM
    high = (head_index + 1) * group_size * HEAD_DIM
    grad_head = jnp.where(live_rows[:, None], grad_rows[:, low:high], jnp.zeros((), jnp.bfloat16))
    grad_head = grad_head.reshape(row_count, group_size, HEAD_DIM)
    output_head = lax.optimization_barrier(output[:, low:high]).reshape(
        row_count, group_size, HEAD_DIM
    )
    row_dot = jnp.sum(
        grad_head.astype(jnp.float32) * output_head.astype(jnp.float32), axis=2, keepdims=True
    )
    return (grad_head, row_dot)


def backward(
    queries, all_keys, all_values, grad_rows, allowed, live_rows, output, totals, scale_factor
):
    row_count = queries.shape[0]
    kv_count = all_keys.shape[1] // HEAD_DIM
    group_size = queries.shape[1] // all_keys.shape[1]
    query_grads = []
    key_grads = []
    value_grads = []
    for head_index in range(kv_count):
        query_head, key_head, logits = head_logits(
            queries, all_keys, allowed, head_index, group_size, scale_factor
        )
        value_head = all_values[:, head_index * HEAD_DIM : (head_index + 1) * HEAD_DIM]
        prob = jnp.exp(logits - totals[head_index])
        weights = prob.astype(jnp.bfloat16)
        grad_head, row_dot = head_terms(grad_rows, live_rows, output, head_index, group_size)
        spread = jnp.einsum(
            "rhd,kd->rhk", grad_head, value_head, preferred_element_type=jnp.float32
        )
        dlogit = (prob * (spread - row_dot)).astype(jnp.bfloat16)
        query_part = (
            jnp.einsum("rhk,kd->rhd", dlogit, key_head, preferred_element_type=jnp.float32)
            * scale_factor
        )
        query_grads.append(query_part.reshape(row_count, group_size * HEAD_DIM))
        key_grads.append(
            jnp.einsum("rhk,rhd->kd", dlogit, query_head, preferred_element_type=jnp.float32)
            * scale_factor
        )
        value_grads.append(
            jnp.einsum("rhk,rhd->kd", weights, grad_head, preferred_element_type=jnp.float32)
        )
    return (
        jnp.concatenate(query_grads, axis=1),
        jnp.concatenate(key_grads, axis=1),
        jnp.concatenate(value_grads, axis=1),
    )


def body(
    response_query,
    response_key,
    response_value,
    response_grad,
    prompt_key,
    prompt_value,
    lengths,
    home_rank,
    prompt_seen,
):
    rank_count = home_rank.shape[0]
    rank_ids = jnp.arange(rank_count, dtype=jnp.int32)
    resident = jnp.sum(
        jnp.where(home_rank[None, :] == rank_ids[:, None], rank_ids[None, :], 0), axis=1
    )
    own_rank = lax.axis_index("seq")
    scale_factor = 1.0 / HEAD_DIM**0.5
    arrived = (
        lax.all_to_all(response_query[resident], "seq", split_axis=0, concat_axis=1, tiled=True),
        lax.all_to_all(response_key[resident], "seq", split_axis=0, concat_axis=1, tiled=True),
        lax.all_to_all(response_value[resident], "seq", split_axis=0, concat_axis=1, tiled=True),
        lax.all_to_all(response_grad[resident], "seq", split_axis=0, concat_axis=1, tiled=True),
    )
    queries = arrived[0][0]
    own_keys = arrived[1][0]
    own_values = arrived[2][0]
    grad_rows = arrived[3][0]
    own_response = resident[own_rank]
    length = lengths[own_response]
    visible = prompt_seen[own_response]
    max_length = queries.shape[0]
    prompt_rows = prompt_key.shape[0]
    prompt_total = prompt_rows * lax.axis_size("seq")
    positions = jnp.arange(max_length, dtype=jnp.int32)
    prompt_cols = jnp.arange(prompt_total, dtype=jnp.int32)
    seen_part = jnp.broadcast_to(prompt_cols[None, :] < visible, (max_length, prompt_total))
    allowed = jnp.concatenate([seen_part, positions[None, :] <= positions[:, None]], axis=1)
    live_rows = positions < length
    gathered_keys, gathered_values = (
        lax.all_gather(prompt_key, "seq", axis=0, tiled=True),
        lax.all_gather(prompt_value, "seq", axis=0, tiled=True),
    )
    all_keys = jnp.concatenate([gathered_keys, own_keys], axis=0)
    all_values = jnp.concatenate([gathered_values, own_values], axis=0)
    response_out, response_totals = forward(
        queries, all_keys, all_values, allowed, live_rows, scale_factor
    )
    query_grad, key_grad, value_grad = backward(
        queries,
        all_keys,
        all_values,
        grad_rows,
        allowed,
        live_rows,
        response_out,
        response_totals,
        scale_factor,
    )
    key_summed, value_summed = (
        lax.psum_scatter(key_grad[:prompt_total], "seq", scatter_dimension=0, tiled=True),
        lax.psum_scatter(value_grad[:prompt_total], "seq", scatter_dimension=0, tiled=True),
    )
    returned = (
        lax.all_to_all(
            query_grad.astype(jnp.bfloat16)[None], "seq", split_axis=1, concat_axis=0, tiled=True
        ),
        lax.all_to_all(
            key_grad[prompt_total:].astype(jnp.bfloat16)[None],
            "seq",
            split_axis=1,
            concat_axis=0,
            tiled=True,
        ),
        lax.all_to_all(
            value_grad[prompt_total:].astype(jnp.bfloat16)[None],
            "seq",
            split_axis=1,
            concat_axis=0,
            tiled=True,
        ),
    )
    return (
        response_out[None],
        returned[0][home_rank],
        returned[1][home_rank],
        returned[2][home_rank],
        key_summed.astype(jnp.bfloat16),
        value_summed.astype(jnp.bfloat16),
    )


def choose_body(response_query, *others):
    count, rows = response_query.shape[:2]
    prompt_rows = others[3].shape[0]
    fits = rows % 16 == 0 and prompt_rows <= rows and rows * count == HEAD_DIM
    if fits and count in (4, 8):
        return packed_body(response_query, *others)
    return body(response_query, *others)


def solution(mesh):
    placed = (
        P("group", "seq", "head"),
        P("group", "seq", "head"),
        P("group", "seq", "head"),
        P("group", "seq", "head"),
        P(("group", "seq"), "head"),
        P(("group", "seq"), "head"),
        P("group"),
        P("group"),
        P("group"),
    )
    return jax.shard_map(
        choose_body,
        mesh=mesh,
        in_specs=placed,
        out_specs=(
            P(("group", "seq"), None, "head"),
            P("group", "seq", "head"),
            P("group", "seq", "head"),
            P("group", "seq", "head"),
            P(("group", "seq"), "head"),
            P(("group", "seq"), "head"),
        ),
        check_vma=False,
    )
```
